512 devices in a mesh: row: 32 (over z, core), col: 16 (over x, y).
Axes of the slice: x: 4, y: 4, z: 16, core: 2. Of those that a mesh axis runs over, the one named last changes fastest.
Arguments:
- factor: bfloat16 [8192, 8192], P('row', 'col'), as said below
- sel_tiles: int32 [32], replicated, may hold values from 0 to 63, as said below
- coupling: bfloat16 [8192, 2048], P('col', 'row')
Outputs:
- root_inverse: float32 [8192, 8192], P('row', 'col')
- child_inverse: float32 [2048, 8192], P('col', 'row')
The draws below stay inside these ranges and needn't reach their ends.
Inputs may be any that keep to these rules, and one draw needn't show every extreme that they name: sel_tiles holds 32 distinct tile indices in increasing order; rows of coupling outside the listed tiles are zero. factor is lower triangular with a diagonal between 1 and 1.5.
All inputs are finite; a program needn't handle non-finite values.
Results may differ from the reference program's by a relative error of at most 0.003.
Values may be sent and summed in bfloat16 or wider, within the bound.
A program may use at most 64 MiB of HBM per device.

```python
import jax
import jax.numpy as jnp

S = 8192
TILE = 128
NCH = 2048
R = 32


def chosen_tiles(key):
    order = jax.random.permutation(jax.random.fold_in(key, 7), S // TILE)
    return jnp.sort(order[:R]).astype(jnp.int32)


def draw_sel_tiles(key, part):
    return chosen_tiles(key)


def draw_factor(key, part):
    first = jax.random.fold_in(key, 11)
    second = jax.random.fold_in(key, 13)
    rows = jnp.arange(S)[:, None]
    cols = jnp.arange(S)[None, :]
    lower = jax.random.normal(first, (S, S), jnp.float32)
    lower = lower * S ** (-0.5)
    diag = 1.0 + 0.5 * jax.random.uniform(second, (S,), jnp.float32)
    full = jnp.where(rows > cols, lower, 0.0) + jnp.where(rows == cols, diag[None, :], 0.0)
    return full.astype(jnp.bfloat16)


def draw_coupling(key, part):
    tiles = chosen_tiles(key)
    tile_of = (jnp.arange(S) // TILE).astype(jnp.int32)
    member = jnp.any(tile_of[:, None] == tiles[None, :], axis=1)
    values = 0.5 * jax.random.normal(jax.random.fold_in(key, 5), (S, NCH), jnp.float32)
    return jnp.where(member[:, None], values, 0.0).astype(jnp.bfloat16)


def setup_inputs(seed: int = 0) -> dict:
    key_of = jax.random.split(jax.random.key(seed), 4)
    factor = draw_factor(jax.random.fold_in(key_of[3], 71), 0)
    sel_tiles = draw_sel_tiles(jax.random.fold_in(key_of[3], 71), 0)
    coupling = draw_coupling(jax.random.fold_in(key_of[3], 71), 0)
    return {"factor": factor, "sel_tiles": sel_tiles, "coupling": coupling}


def reference(factor, sel_tiles, coupling):
    gram = jnp.dot(factor.T, factor, preferred_element_type=jnp.float32)
    rounded = gram.astype(jnp.bfloat16)
    tile_of = (jnp.arange(S) // TILE).astype(jnp.int32)
    member = jnp.any(tile_of[:, None] == sel_tiles[None, :], axis=1)
    product = jnp.dot(coupling.T, rounded.T, preferred_element_type=jnp.float32)
    child = jnp.where(member[None, :], -product, jnp.float32(0.0))
    return gram, child
```

```python
import functools

import jax
import jax.numpy as jnp
from jax import lax
from jax.experimental import pallas as pl
from jax.experimental.pallas import tpu as pltpu
from jax.sharding import PartitionSpec as P

TILE = 128
MESH = pl.DeviceIdType.MESH
F32 = jnp.float32
BF16 = jnp.bfloat16
SIDE = 4


def kernel(
    blk_ref, w_hbm, g_ref, child_ref,
    panel, tp, gb, part, parts_in,
    ring_send, ring_recv, pair_send, pair_recv, own_send, own_recv,
    t_send, t_recv, local_sem, p1_send, p1_recv, p2_send, p2_recv, rs_send, rs_recv,
):
    row = lax.axis_index("row")
    col = lax.axis_index("col")
    rows = lax.axis_size("row")
    cols = lax.axis_size("col")
    core = lax.rem(row, 2)
    z = row // 2
    x = col // SIDE
    y = lax.rem(col, SIDE)
    partner = row + 1 - 2 * core
    up = lax.rem(row + 2, rows)
    down = lax.rem(row + rows - 2, rows)
    diagonal = z == col
    wr, wc = w_hbm.shape
    half = wc // 2
    chunk = blk_ref.shape[0] // 2

    def copy(src, dst, ssem, rsem, r, c):
        return pltpu.make_async_remote_copy(
            src_ref=src, dst_ref=dst, send_sem=ssem, recv_sem=rsem,
            device_id=(r, c), device_id_type=MESH,
        )

    barrier = pltpu.get_barrier_semaphore()

    def greet(r, c):
        pl.semaphore_signal(barrier, inc=1, device_id=(r, c), device_id_type=MESH)

    for r in (up, down, partner):
        greet(r, col)
    for d in range(1, cols):
        greet(row, lax.rem(col + d, cols))
    @pl.when(jnp.logical_not(diagonal))
    def _():
        greet(2 * col, z)
        greet(2 * col + 1, z)

    pl.semaphore_wait(barrier, cols - 1 + 3 + jnp.where(diagonal, 0, 2))

    rows_of = lambda h: pl.ds(h * chunk, chunk)

    def ring(direction, step, h, src, slot):
        return copy(
            src, panel.at[slot, rows_of(h)],
            ring_send.at[direction, step, h], ring_recv.at[direction, step, h],
            up if direction == 0 else down, col,
        )

    def to_pair(direction, step, h, slot):
        return copy(
            panel.at[slot, rows_of(h)], panel.at[slot, rows_of(h)],
            pair_send.at[direction, step, h], pair_recv.at[direction, step, h],
            partner, col,
        )

    def own_pair(h):
        return copy(
            blk_ref.at[rows_of(h)], panel.at[row, rows_of(h)],
            own_send.at[h], own_recv.at[h], partner, col,
        )

    for h in range(2):
        for direction in range(2):
            ring(direction, 0, h, blk_ref.at[rows_of(h)], row).start()

    def mirrored(k):
        return copy(
            blk_ref.at[pl.ds(0, wr), pl.ds(k * half, half)],
            tp.at[z, pl.ds(pl.multiple_of(core * wr, wr), wr)],
            t_send.at[k], t_recv.at[core], 2 * col + k, z,
        )

    local = pltpu.make_async_copy(
        w_hbm.at[:, pl.ds(pl.multiple_of(core * half, half), half)],
        tp.at[col, pl.ds(pl.multiple_of(core * wr, wr), wr)],
        local_sem,
    )
    for k in range(2):
        mine = jnp.logical_and(diagonal, core == k)

        @pl.when(jnp.logical_not(mine))
        def _():
            mirrored(k).start()

    @pl.when(diagonal)
    def _():
        local.start()

    for h in range(2):
        own_pair(h).start()
    panel[row] = blk_ref[...]

    steps = rows // 4

    def ring_step(s):
        for h in range(2):
            for direction in range(2):
                off = 2 * s
                slot = lax.rem(row + (rows - off if direction == 0 else off), rows)

                def handle():
                    ring(direction, s - 1, h, panel.at[slot, rows_of(h)], slot).wait_recv()

                    @pl.when(jnp.logical_or(s + 1 < steps, jnp.logical_and(s + 1 == steps, h == direction)))
                    def _():
                        ring(direction, s, h, panel.at[slot, rows_of(h)], slot).start()

                    to_pair(direction, s - 1, h, slot).start()

                @pl.when(jnp.logical_or(s < steps, h == direction))
                def _():
                    handle()

    def ring_range(a, b):
        def step(s, carry):
            ring_step(s)
            return carry

        lax.fori_loop(a, b, step, 0)

    ring_range(1, 3)

    def part_rows(k):
        return pl.ds(k * wr, wr)

    for k in range(2):
        here = jnp.logical_and(diagonal, core == k)

        @pl.when(jnp.logical_not(here))
        def _():
            copy(
                blk_ref.at[pl.ds(0, wr), pl.ds(0, half)], tp.at[col, part_rows(k)],
                t_send.at[k], t_recv.at[k], 2 * col + k, z,
            ).wait_recv()

    @pl.when(diagonal)
    def _():
        local.wait()

    def moved(k, d):
        if k == 0:
            return lax.rem(x + d, SIDE) * SIDE + y
        return x * SIDE + lax.rem(y + d, SIDE)

    def first(k, d, slot):
        return copy(
            tp.at[slot, part_rows(k)], tp.at[slot, part_rows(k)],
            p1_send.at[k, d - 1], p1_recv.at[k, d - 1], row, moved(k, d),
        )

    def second(k, e, d, slot):
        return copy(
            tp.at[slot, part_rows(k)], tp.at[slot, part_rows(k)],
            p2_send.at[k, e, d - 1], p2_recv.at[k, e, d - 1], row, moved(1 - k, d),
        )

    order = (1, 3, 2)
    for d in order:
        for k in range(2):
            first(k, d, col).start()
    for d in order:
        for k in range(2):
            second(k, 0, d, col).start()
    ring_range(3, 5)
    for e in order:
        for k in range(2):
            slot = moved(k, SIDE - e)
            first(k, e, slot).wait_recv()
            for d in order:
                second(k, e, d, slot).start()
    ring_range(5, steps + 1)

    for e in range(SIDE):
        for k in range(2):
            for d in order:
                second(k, e, d, col).wait_recv()
    for h in range(2):
        own_pair(h).wait_recv()
    for s in range(1, steps + 1):
        for h in range(2):
            for direction in range(2):
                if s < steps or h == direction:
                    to_pair(direction, s - 1, h, row).wait_recv()

    def add(m, carry):
        left = tp[m]
        right = panel[pl.ds(2 * m, 2), pl.ds(0, wr)].reshape(2 * wr, wc)
        prod = lax.dot_general(left, right, (((0,), (0,)), ((), ())), preferred_element_type=F32)

        @pl.when(m == 0)
        def _():
            g_ref[...] = prod

        @pl.when(m > 0)
        def _():
            g_ref[...] += prod

        return carry

    lax.fori_loop(0, cols, add, 0)
    gb[...] = g_ref[...].astype(BF16)

    def child_part(c, carry):
        cpl = panel[pl.ds(2 * c, 2), pl.ds(wr, blk_ref.shape[0] - wr)].reshape(part.shape[1], wc)
        part[c] = lax.dot_general(
            cpl, gb[...], (((1,), (1,)), ((), ())), preferred_element_type=F32
        ).astype(BF16)
        return carry

    lax.fori_loop(0, cols, child_part, 0)

    def scatter(d):
        to = lax.rem(col + d, cols)
        return copy(part.at[to], parts_in.at[col], rs_send.at[d - 1], rs_recv.at[d - 1], row, to)

    for d in range(1, cols):
        scatter(d).start()
    child_ref[...] = -part[col].astype(F32)
    for d in range(1, cols):
        scatter(d).wait_recv()
        child_ref[...] -= parts_in[lax.rem(col + cols - d, cols)].astype(F32)

    for h in range(2):
        own_pair(h).wait_send()
    for s in range(0, steps):
        for h in range(2):
            for direction in range(2):
                if s + 1 < steps or h == direction:
                    ring(direction, s, h, blk_ref.at[rows_of(h)], row).wait_send()
                    to_pair(direction, s, h, row).wait_send()
    for k in range(2):
        mine = jnp.logical_and(diagonal, core == k)

        @pl.when(jnp.logical_not(mine))
        def _():
            mirrored(k).wait_send()

    for k in range(2):
        for d in order:
            first(k, d, col).wait_send()
            for e in range(SIDE):
                second(k, e, d, col).wait_send()
    for d in range(1, cols):
        scatter(d).wait_send()


def body(factor, sel_tiles, coupling):
    rows, cols = lax.axis_size("row"), lax.axis_size("col")
    wr, wc = factor.shape
    kc = coupling.shape[1]
    row_index = lax.axis_index("row")
    blk = jnp.concatenate([factor, coupling.T], axis=0)
    kb = rows * kc // cols
    dma = pltpu.SemaphoreType.DMA
    vm = pl.BlockSpec(memory_space=pltpu.VMEM)
    steps = rows // 4
    gram, child = pl.pallas_call(
        kernel,
        out_shape=(
            jax.ShapeDtypeStruct((wr, wc), F32),
            jax.ShapeDtypeStruct((kb, wr), F32),
        ),
        in_specs=[vm, pl.BlockSpec(memory_space=pl.ANY)],
        out_specs=(vm, vm),
        scratch_shapes=[
            pltpu.VMEM((rows, wr + kc, wc), BF16),
            pltpu.VMEM((cols, 2 * wr, wc // 2), BF16),
            pltpu.VMEM((wr, wc), BF16),
            pltpu.VMEM((cols, kb, wr), BF16),
            pltpu.VMEM((cols, kb, wr), BF16),
            dma((2, steps, 2)), dma((2, steps, 2)),
            dma((2, steps, 2)), dma((2, steps, 2)),
            dma((2,)), dma((2,)),
            dma((2,)), dma((2,)), dma,
            dma((2, SIDE - 1)), dma((2, SIDE - 1)),
            dma((2, SIDE, SIDE - 1)), dma((2, SIDE, SIDE - 1)),
            dma((cols - 1,)), dma((cols - 1,)),
        ],
        compiler_params=pltpu.CompilerParams(
            collective_id=0, has_side_effects=True, vmem_limit_bytes=48 * 2**20
        ),
    )(blk, factor)
    global_rows = row_index * wr + jnp.arange(wr, dtype=jnp.int32)
    member = jnp.any((global_rows // TILE)[:, None] == sel_tiles[None, :], axis=1)
    return gram, jnp.where(member[None, :], child, jnp.float32(0.0))


def solution(mesh):
    return jax.shard_map(
        body,
        mesh=mesh,
        in_specs=(P("row", "col"), P(), P("col", "row")),
        out_specs=(P("row", "col"), P("col", "row")),
        check_vma=False,
    )
```

```python
import jax
import jax.numpy as jnp
from jax import lax
from jax.experimental import pallas as pl
from jax.experimental.pallas import tpu as pltpu
from jax.sharding import PartitionSpec as P

TILE = 128
MESH = pl.DeviceIdType.MESH
F32 = jnp.float32
BF16 = jnp.bfloat16
SIDE = 4
N = SIDE * SIDE
FAR = N // 2
CUTS = 2
HOPS = 8
EARLY = 6


def both(*conditions):
    out = conditions[0]
    for c in conditions[1:]:
        out = jnp.logical_and(out, c)
    return out


def kernel(
    w_ref, ut_ref, w_hbm, g_ref, child_ref,
    panel, upanel, tp, stage, gb, part, parts_in,
    ring_send, ring_recv, u_send, u_recv, pair_send, pair_recv, upair_send, upair_recv,
    own_send, own_recv,
    leg1_send, leg1_recv, leg2_send, leg2_recv, local_sem,
    p1_send, p1_recv, p2_send, p2_recv, rs_send, rs_recv,
):
    row = lax.axis_index("row")
    col = lax.axis_index("col")
    rows = 2 * N
    core = lax.rem(row, 2)
    z = row // 2
    x = col // SIDE
    y = lax.rem(col, SIDE)
    other = 1 - core
    partner = 2 * z + other
    up = lax.rem(row + 2, rows)
    down = lax.rem(row + rows - 2, rows)
    wr, wc = w_ref.shape
    half = wc // 2
    chunk = wr // CUTS

    def copy(src, dst, ssem, rsem, r, c):
        return pltpu.make_async_remote_copy(
            src_ref=src, dst_ref=dst, send_sem=ssem, recv_sem=rsem,
            device_id=(r, c), device_id_type=MESH,
        )

    reach = FAR

    def travels(m, direction, s, h):
        high = m >= N - reach
        if direction == 0:
            near = s < N - reach if h % 2 else s <= N - reach
            return both(m >= col, high, near)
        near = s <= reach if h % 2 else s < reach
        return both(m >= col, s <= m, jnp.logical_or(jnp.logical_not(high), near))

    def comes_at(m):
        down_only = jnp.logical_or(m < N - reach, m - z < reach)
        return jnp.where(down_only, m - z, N - (m - z))

    def wanted(m):
        return both(m >= col, m >= z)

    def origin(direction, s):
        return lax.rem(z + (N - s if direction == 0 else s), N)

    barrier = pltpu.get_barrier_semaphore()

    def greet(r, c):
        pl.semaphore_signal(barrier, inc=1, device_id=(r, c), device_id_type=MESH)

    turn = lax.rem(col + 2 * N - z - FAR * core, N)
    for r in (up, down, partner):
        greet(r, col)
    for d in range(1, N):
        greet(row, lax.rem(col + d, N))
    greet(partner, turn)

    @pl.when(turn != z)
    def _():
        greet(2 * turn + core, col)

    with jax.named_scope("barrier"):
        pl.semaphore_wait(barrier, N + 3 + jnp.where(turn != z, 1, 0))

    def rows_of(h):
        return pl.ds(h * chunk, chunk)

    def towards(direction):
        return up if direction == 0 else down

    def slot_of(m):
        return 2 * m + core

    def hop(direction, s, h, m, first):
        dst = panel.at[slot_of(m), rows_of(h)]
        return copy(
            w_ref.at[rows_of(h)] if first else dst, dst,
            ring_send.at[direction, s - 1, h], ring_recv.at[direction, s - 1, h], towards(direction), col,
        )

    def u_hop(direction, s, m, first):
        dst = upanel.at[slot_of(m)]
        return copy(
            ut_ref if first else dst, dst, u_send.at[direction, s - 1], u_recv.at[direction, s - 1],
            towards(direction), col,
        )

    def to_pair(direction, s, h, m):
        ref = panel.at[slot_of(m), rows_of(h)]
        return copy(
            ref, ref, pair_send.at[direction, s - 1, h], pair_recv.at[direction, s - 1, h], partner, col
        )

    def u_pair(direction, s, m):
        ref = upanel.at[slot_of(m)]
        return copy(ref, ref, upair_send.at[direction, s - 1], upair_recv.at[direction, s - 1], partner, col)

    def own_pair(k):
        src, dst = ((w_ref, panel), (ut_ref, upanel))[k]
        return copy(src, dst.at[row], own_send.at[k], own_recv.at[k], partner, col)

    def part_rows(k):
        return pl.ds(k * wr, wr)

    my_rows = pl.ds(pl.multiple_of(core * wr, wr), wr)

    def leg1(k, dst):
        to = lax.rem(z + col + FAR * k, N)
        return copy(
            w_ref.at[:, pl.ds(k * half, half)], dst, leg1_send.at[k], leg1_recv.at[core], 2 * z + k, to
        )

    def leg1_local(dst):
        return pltpu.make_async_copy(
            w_hbm.at[:, pl.ds(pl.multiple_of(core * half, half), half)], dst, local_sem
        )

    def leg1_self(k):
        return both(core == k, lax.rem(z + FAR * k, N) == 0)

    def leg2():
        return copy(stage, tp.at[z], leg2_send, leg2_recv, 2 * turn + core, col)

    for h in range(CUTS):
        for direction in range(2):
            @pl.when(travels(z, direction, 1, h))
            def _():
                hop(direction, 1, h, z, True).start()

    for k in range(2):
        for at_home in (False, True):
            dst = tp.at[z, my_rows] if at_home else stage.at[my_rows]
            good = both(z >= col, (z == col) == at_home)

            @pl.when(both(good, jnp.logical_not(leg1_self(k))))
            def _():
                leg1(k, dst).start()

            @pl.when(both(good, leg1_self(k)))
            def _():
                leg1_local(dst).start()

    for direction in range(2):
        u_hop(direction, 1, z, True).start()
    for k in range(2):
        own_pair(k).start()
    panel[row] = w_ref[...]
    upanel[row] = ut_ref[...]
    g_ref[...] = jnp.zeros_like(g_ref)

    def leg1_arrived():
        for k in range(2):
            here = both(turn == col, core == k)

            @pl.when(here)
            def _():
                leg1_local(stage.at[part_rows(k)]).wait()

            @pl.when(jnp.logical_not(here))
            def _():
                copy(
                    w_ref.at[:, pl.ds(0, half)], stage.at[part_rows(k)], leg1_send.at[k], leg1_recv.at[k],
                    row, col,
                ).wait_recv()

    def passes(s):
        for h in range(CUTS):
            for direction in range(2):
                m = origin(direction, s)

                @pl.when(travels(m, direction, s, h))
                def _():
                    hop(direction, s, h, m, False).wait_recv()

                    @pl.when(both(s < HOPS, travels(m, direction, s + 1, h)))
                    def _():
                        hop(direction, s + 1, h, m, False).start()

                    @pl.when(wanted(m))
                    def _():
                        to_pair(direction, s, h, m).start()

    def u_passes(s):
        for direction in range(2):
            m = origin(direction, s)

            @pl.when(s < FAR + 1 - direction)
            def _():
                u_hop(direction, s, m, False).wait_recv()

                @pl.when(s < FAR - direction)
                def _():
                    u_hop(direction, s + 1, m, False).start()

                u_pair(direction, s, m).start()

    def ring_step(s, carry):
        passes(s)
        u_passes(s)
        return carry

    def ring_range(a, b):
        with jax.named_scope("ring%d" % a):
            lax.fori_loop(a, b, ring_step, 0)

    ring_range(1, 2)

    @pl.when(z >= turn)
    def _():
        with jax.named_scope("leg1"):
            leg1_arrived()

        @pl.when(z > turn)
        def _():
            leg2().start()

    ring_range(2, 4)

    def moved(k, d):
        if k == 0:
            return lax.rem(x + d, SIDE) * SIDE + y
        return x * SIDE + lax.rem(y + d, SIDE)

    def row_of(c):
        return lax.rem(c + 2 * N - z - FAR * core, N)

    def least(k, c):
        return c // SIDE * SIDE if k == 0 else lax.rem(c, SIDE)

    def first(k, d, m):
        ref = tp.at[m, part_rows(k)]
        return copy(ref, ref, p1_send.at[k, d - 1], p1_recv.at[k, d - 1], row, moved(k, d))

    def second(k, e, d, m):
        ref = tp.at[m, part_rows(k)]
        return copy(ref, ref, p2_send.at[k, e, d - 1], p2_recv.at[k, e, d - 1], row, moved(1 - k, d))

    def first_goes(k, m, c):
        return both(m >= z, m >= least(k, c))

    def second_goes(m, c):
        return both(m >= z, m >= c)

    order = (1, 3, 2)
    mine = turn

    @pl.when(mine > z)
    def _():
        with jax.named_scope("leg2"):
            copy(stage, tp.at[mine], leg2_send, leg2_recv, row, col).wait_recv()

    for d in order:
        for k in range(2):
            @pl.when(first_goes(k, mine, moved(k, d)))
            def _():
                first(k, d, mine).start()
    for d in order:
        for k in range(2):
            @pl.when(second_goes(mine, moved(1 - k, d)))
            def _():
                second(k, 0, d, mine).start()

    ring_range(4, 6)

    for e in order:
        for k in range(2):
            m = row_of(moved(k, SIDE - e))

            @pl.when(first_goes(k, m, col))
            def _():
                with jax.named_scope("first%d%d" % (k, e)):
                    first(k, e, m).wait_recv()
                for d in order:
                    @pl.when(second_goes(m, moved(1 - k, d)))
                    def _():
                        second(k, e, d, m).start()

    ring_range(6, EARLY + 2)

    with jax.named_scope("second"):
        for e in range(SIDE):
            for k in range(2):
                for d in order:
                    a, b = (e, d) if k == 0 else (d, e)
                    c = lax.rem(x + SIDE - a, SIDE) * SIDE + lax.rem(y + SIDE - b, SIDE)
                    m = row_of(c)

                    @pl.when(second_goes(m, col))
                    def _():
                        second(k, e, d, m).wait_recv()

    def pairs(s, carry):
        for h in range(CUTS):
            for direction in range(2):
                m = origin(direction, s)

                @pl.when(both(travels(m, direction, s, h), wanted(m)))
                def _():
                    to_pair(direction, s, h, m).wait_recv()

        return carry

    def add(m):
        left = tp[m]
        right = panel[pl.ds(2 * m, 2)].reshape(2 * wr, wc)
        g_ref[...] += lax.dot_general(left, right, (((0,), (0,)), ((), ())), preferred_element_type=F32)

    with jax.named_scope("pairs"):
        for k in range(2):
            own_pair(k).wait_recv()
        lax.fori_loop(1, EARLY + 1, pairs, 0)

    def add_blocks(early):
        def step(m, carry):
            @pl.when(both(wanted(m), (comes_at(m) <= EARLY) == early))
            def _():
                add(m)

            return carry

        lax.fori_loop(0, N, step, 0)

    with jax.named_scope("gram"):
        add_blocks(True)

    ring_range(EARLY + 2, HOPS + 1)

    with jax.named_scope("last"):
        lax.fori_loop(EARLY + 1, HOPS + 1, pairs, 0)
        add_blocks(False)
        for direction in range(2):
            for s in range(1, FAR + 1 - direction):
                u_pair(direction, s, origin(direction, s)).wait_recv()
    gb[...] = jnp.transpose(g_ref[...].astype(BF16))

    def child_part(c, carry):
        cpl = upanel[pl.ds(8 * c, 8)].reshape(4 * part.shape[1], wc)
        prod = jnp.dot(cpl, gb[...], preferred_element_type=F32).astype(BF16)
        part[pl.ds(4 * c, 4)] = prod.reshape(4, *part.shape[1:])
        return carry

    with jax.named_scope("child"):
        lax.fori_loop(0, N // 4, child_part, 0)

    def scatter(d):
        to = lax.rem(col + d, N)
        return copy(part.at[to], parts_in.at[col], rs_send.at[d - 1], rs_recv.at[d - 1], row, to)

    for d in range(1, N):
        scatter(d).start()
    def sent(s, carry):
        for direction in range(2):
            m = origin(direction, s - 1)
            got = origin(direction, s)
            for h in range(CUTS):
                @pl.when(travels(m, direction, s, h))
                def _():
                    hop(direction, s, h, m, False).wait_send()

                @pl.when(both(travels(got, direction, s, h), wanted(got)))
                def _():
                    to_pair(direction, s, h, got).wait_send()

            @pl.when(s < FAR + 1 - direction)
            def _():
                u_hop(direction, s, m, False).wait_send()
                u_pair(direction, s, got).wait_send()

        return carry

    with jax.named_scope("sends"):
        lax.fori_loop(1, HOPS + 1, sent, 0)
        for k in range(2):
            own_pair(k).wait_send()

            @pl.when(both(z >= col, jnp.logical_not(leg1_self(k))))
            def _():
                leg1(k, stage.at[my_rows]).wait_send()

            for d in order:
                @pl.when(first_goes(k, mine, moved(k, d)))
                def _():
                    first(k, d, mine).wait_send()

                for e in range(SIDE):
                    m = row_of(moved(k, SIDE - e if e else 0))
                    reaches = second_goes(m, moved(1 - k, d))

                    @pl.when(reaches)
                    def _():
                        second(k, e, d, m).wait_send()

        @pl.when(z > turn)
        def _():
            leg2().wait_send()


    with jax.named_scope("scatter"):
        child_ref[...] = -part[col].astype(F32)
        for d in range(1, N):
            scatter(d).wait_recv()
            child_ref[...] -= parts_in[lax.rem(col + N - d, N)].astype(F32)
        for d in range(1, N):
            scatter(d).wait_send()


def body(factor, sel_tiles, coupling):
    rows, cols = lax.axis_size("row"), lax.axis_size("col")
    assert rows == 2 * N and cols == N
    wr, wc = factor.shape
    kc = coupling.shape[1]
    row_index = lax.axis_index("row")
    kb = rows * kc // cols
    dma = pltpu.SemaphoreType.DMA
    vm = pl.BlockSpec(memory_space=pltpu.VMEM)
    pair_of = lambda *shape: [dma(shape), dma(shape)]
    gram, child = pl.pallas_call(
        kernel,
        out_shape=(
            jax.ShapeDtypeStruct((wr, wc), F32),
            jax.ShapeDtypeStruct((kb, wr), F32),
        ),
        in_specs=[vm, vm, pl.BlockSpec(memory_space=pl.ANY)],
        out_specs=(vm, vm),
        scratch_shapes=[
            pltpu.VMEM((rows, wr, wc), BF16),
            pltpu.VMEM((rows, kc, wc), BF16),
            pltpu.VMEM((cols, 2 * wr, wc // 2), BF16),
            pltpu.VMEM((2 * wr, wc // 2), BF16),
            pltpu.VMEM((wc, wr), BF16),
            pltpu.VMEM((cols, kb, wr), BF16),
            pltpu.VMEM((cols, kb, wr), BF16),
            *pair_of(2, HOPS, CUTS), *pair_of(2, FAR), *pair_of(2, HOPS, CUTS), *pair_of(2, FAR),
            *pair_of(2),
            *pair_of(2), dma, dma, dma,
            *pair_of(2, SIDE - 1), *pair_of(2, SIDE, SIDE - 1), *pair_of(cols - 1),
        ],
        compiler_params=pltpu.CompilerParams(
            collective_id=0, has_side_effects=True, vmem_limit_bytes=52 * 2**20
        ),
    )(factor, coupling.T, factor)
    global_rows = row_index * wr + jnp.arange(wr, dtype=jnp.int32)
    member = jnp.any((global_rows // TILE)[:, None] == sel_tiles[None, :], axis=1)
    return gram, jnp.where(member[None, :], child, jnp.float32(0.0))


def solution(mesh):
    return jax.shard_map(
        body,
        mesh=mesh,
        in_specs=(P("row", "col"), P(), P("col", "row")),
        out_specs=(P("row", "col"), P("col", "row")),
        check_vma=False,
    )
```

```python
import jax
import jax.numpy as jnp
from jax import lax
from jax.experimental import pallas as pl
from jax.experimental.pallas import tpu as pltpu
from jax.sharding import PartitionSpec as P

TILE = 128
MESH = pl.DeviceIdType.MESH
F32 = jnp.float32
BF16 = jnp.bfloat16
SIDE = 4
N = SIDE * SIDE
FAR = N // 2
CUTS = 2
HOPS = FAR
NEAR = 4
MIRRORED = 4
EARLY = 5


def both(*conditions):
    out = conditions[0]
    for c in conditions[1:]:
        out = jnp.logical_and(out, c)
    return out


def kernel(
    w_ref, ut_ref, member_ref, g_ref, child_ref,
    panel, upanel, tp, stage, gb, part, sums, mids, row_in, last_in,
    ring_send, ring_recv, u_send, u_recv, pair_send, pair_recv, upair_send, upair_recv,
    own_send, own_recv,
    leg1_send, leg1_recv, leg2_send, leg2_recv, hand_send, hand_recv, hand_own,
    p1_send, p1_recv, p2_send, p2_recv, r1_send, r1_recv, r2_send, r2_recv,
):
    row = lax.axis_index("row")
    col = lax.axis_index("col")
    rows = 2 * N
    core = lax.rem(row, 2)
    z = row // 2
    x = col // SIDE
    y = lax.rem(col, SIDE)
    other = 1 - core
    partner = 2 * z + other
    up = lax.rem(row + 2, rows)
    down = lax.rem(row + rows - 2, rows)
    wr, wc = w_ref.shape
    half = wc // 2
    chunk = wr // CUTS

    def copy(src, dst, ssem, rsem, r, c):
        return pltpu.make_async_remote_copy(
            src_ref=src, dst_ref=dst, send_sem=ssem, recv_sem=rsem,
            device_id=(r, c), device_id_type=MESH,
        )

    def travels(m, direction, s, h):
        near = jnp.logical_or(s < FAR, h % 2 == direction)
        return both(m >= col, m >= FAR if direction == 0 else s <= m, near)

    def gap(m, plane):
        return jnp.where(m - plane <= FAR, m - plane, N - (m - plane))

    def comes_at(m):
        return gap(m, z)

    def wanted(m):
        return both(m >= col, m >= z)

    def origin(direction, s):
        return lax.rem(z + (N - s if direction == 0 else s), N)

    barrier = pltpu.get_barrier_semaphore()

    def greet(r, c):
        pl.semaphore_signal(barrier, inc=1, device_id=(r, c), device_id_type=MESH)

    turn = lax.rem(col + 2 * N - z - FAR * core, N)
    for r in (up, down, partner):
        greet(r, col)
    for d in range(1, N):
        greet(row, lax.rem(col + d, N))
    greet(partner, turn)

    @pl.when(turn != z)
    def _():
        greet(2 * turn + core, col)

    @pl.when(col != z)
    def _():
        greet(partner, z)

    with jax.named_scope("barrier"):
        pl.semaphore_wait(barrier, N + 3 + jnp.where(turn != z, 1, 0) + jnp.where(col == z, N - 1, 0))

    def rows_of(h):
        return pl.ds(h * chunk, chunk)

    def towards(direction):
        return up if direction == 0 else down

    def slot_of(m):
        return 2 * m + core

    def hop(direction, s, h, m, first):
        dst = panel.at[slot_of(m), rows_of(h)]
        return copy(
            w_ref.at[rows_of(h)] if first else dst, dst,
            ring_send.at[direction, s - 1, h], ring_recv.at[direction, s - 1, h], towards(direction), col,
        )

    def u_hop(direction, s, m, first):
        dst = upanel.at[slot_of(m)]
        return copy(
            ut_ref if first else dst, dst, u_send.at[direction, s - 1], u_recv.at[direction, s - 1],
            towards(direction), col,
        )

    def to_pair(direction, s, h, m):
        ref = panel.at[slot_of(m), rows_of(h)]
        return copy(
            ref, ref, pair_send.at[direction, s - 1, h], pair_recv.at[direction, s - 1, h], partner, col
        )

    def u_pair(direction, s, m):
        ref = upanel.at[slot_of(m)]
        return copy(ref, ref, upair_send.at[direction, s - 1], upair_recv.at[direction, s - 1], partner, col)

    def own_pair(k):
        src, dst = ((w_ref, panel), (ut_ref, upanel))[k]
        return copy(src, dst.at[row], own_send.at[k], own_recv.at[k], partner, col)

    def part_rows(k):
        return pl.ds(k * wr, wr)

    my_rows = pl.ds(pl.multiple_of(core * wr, wr), wr)

    def leg1(k, dst):
        to = lax.rem(z + col + FAR * k, N)
        return copy(
            w_ref.at[:, pl.ds(k * half, half)], dst, leg1_send.at[k], leg1_recv.at[core], 2 * z + k, to
        )

    def stays(k, m):
        return both(core == k, lax.rem(m + FAR * k, N) == 0)

    def mirrors(m, plane):
        return both(m >= plane, gap(m, plane) > NEAR)

    def leg2():
        return copy(stage, tp.at[z], leg2_send, leg2_recv, 2 * turn + core, col)

    for h in range(CUTS):
        for direction in range(2):
            @pl.when(travels(z, direction, 1, h))
            def _():
                hop(direction, 1, h, z, True).start()

    for k in range(2):
        @pl.when(both(mirrors(z, col), jnp.logical_not(stays(k, z))))
        def _():
            leg1(k, stage.at[my_rows]).start()

        @pl.when(both(mirrors(z, col), stays(k, z)))
        def _():
            stage[my_rows] = w_ref[:, pl.ds(k * half, half)]

    def hand(k, h, m, src, sem):
        return copy(
            src.at[:, pl.ds(k * half, half)],
            tp.at[m, pl.ds(pl.multiple_of(core * wr + h * chunk, chunk), chunk)],
            sem, hand_recv.at[core, h], 2 * z + k, lax.rem(m + z + FAR * k, N),
        )

    def hands(h, m, src, sem_of):
        for k in range(2):
            @pl.when(stays(k, m))
            def _():
                tp[m, pl.ds(pl.multiple_of(core * wr + h * chunk, chunk), chunk)] = src[:, pl.ds(k * half, half)]

            @pl.when(jnp.logical_not(stays(k, m)))
            def _():
                hand(k, h, m, src, sem_of(k)).start()

    @pl.when(col == z)
    def _():
        for h in range(CUTS):
            hands(h, z, w_ref.at[rows_of(h)], lambda k: hand_own.at[h, k])

    for direction in range(2):
        u_hop(direction, 1, z, True).start()
    for k in range(2):
        own_pair(k).start()
    panel[row] = w_ref[...]
    upanel[row] = ut_ref[...]
    g_ref[...] = jnp.zeros_like(g_ref)

    def leg1_arrived():
        for k in range(2):
            @pl.when(jnp.logical_not(both(turn == col, core == k)))
            def _():
                copy(
                    w_ref.at[:, pl.ds(0, half)], stage.at[part_rows(k)], leg1_send.at[k], leg1_recv.at[k],
                    row, col,
                ).wait_recv()

    def moved(k, d):
        if k == 0:
            return lax.rem(x + d, SIDE) * SIDE + y
        return x * SIDE + lax.rem(y + d, SIDE)

    def row_of(c):
        return lax.rem(c + 2 * N - z - FAR * core, N)

    def least(k, c):
        return c // SIDE * SIDE if k == 0 else lax.rem(c, SIDE)

    def first(k, d, m):
        ref = tp.at[m, part_rows(k)]
        return copy(ref, ref, p1_send.at[k, d - 1], p1_recv.at[k, d - 1], row, moved(k, d))

    def second(k, e, d, m):
        ref = tp.at[m, part_rows(k)]
        return copy(ref, ref, p2_send.at[k, e, d - 1], p2_recv.at[k, e, d - 1], row, moved(1 - k, d))

    def first_goes(k, m, c):
        return both(m >= z, m >= least(k, c))

    def second_goes(m, c):
        return both(m >= z, m >= c)

    order = (1, 3, 2)
    mine = turn

    def first_all(action):
        for d in order:
            for k in range(2):
                @pl.when(first_goes(k, mine, moved(k, d)))
                def _():
                    action(first(k, d, mine))

    def second_all(k, e, m, action):
        for d in order:
            @pl.when(second_goes(m, moved(1 - k, d)))
            def _():
                action(second(k, e, d, m))

    def starts_at(m):
        return jnp.where(comes_at(m) <= NEAR, comes_at(m) + 1, MIRRORED)

    def spread(s):
        @pl.when(both(mine >= z, starts_at(mine) == s))
        def _():
            @pl.when(mirrors(mine, z))
            def _():
                copy(stage, tp.at[mine], leg2_send, leg2_recv, row, col).wait_recv()

            for k in range(2):
                @pl.when(jnp.logical_not(jnp.logical_or(mirrors(mine, z), both(col == z, core == k))))
                def _():
                    for h in range(CUTS):
                        pltpu.make_async_remote_copy(
                            src_ref=w_ref.at[rows_of(h), pl.ds(0, half)],
                            dst_ref=tp.at[mine, pl.ds(k * wr + h * chunk, chunk)],
                            send_sem=hand_own.at[h, k], recv_sem=hand_recv.at[k, h],
                            device_id=(partner, col), device_id_type=MESH,
                        ).wait_recv()

            first_all(lambda c: c.start())
            for k in range(2):
                second_all(k, 0, mine, lambda c: c.start())

    def relay(s):
        for e in order:
            for k in range(2):
                m = row_of(moved(k, SIDE - e))

                @pl.when(both(starts_at(m) + 1 == s, first_goes(k, m, col)))
                def _():
                    first(k, e, m).wait_recv()
                    second_all(k, e, m, lambda c: c.start())

    def passes(s):
        for h in range(CUTS):
            for direction in range(2):
                m = origin(direction, s)

                @pl.when(travels(m, direction, s, h))
                def _():
                    hop(direction, s, h, m, False).wait_recv()

                    @pl.when(both(s < HOPS, travels(m, direction, s + 1, h)))
                    def _():
                        hop(direction, s + 1, h, m, False).start()

                    @pl.when(wanted(m))
                    def _():
                        to_pair(direction, s, h, m).start()

                    @pl.when(both(col == z, m >= z, s <= NEAR))
                    def _():
                        src = panel.at[slot_of(m), rows_of(h)]
                        hands(h, m, src, lambda k: hand_send.at[direction, s - 1, h, k])

    def u_passes(s):
        for direction in range(2):
            m = origin(direction, s)

            @pl.when(s < FAR + 1 - direction)
            def _():
                u_hop(direction, s, m, False).wait_recv()

                @pl.when(s < FAR - direction)
                def _():
                    u_hop(direction, s + 1, m, False).start()

                u_pair(direction, s, m).start()

    def ring_step(s, carry):
        passes(s)
        u_passes(s)
        spread(s)
        relay(s)
        return carry

    def ring_range(a, b):
        with jax.named_scope("ring%d" % a):
            lax.fori_loop(a, b, ring_step, 0)

    ring_range(1, 2)

    @pl.when(mirrors(z, turn))
    def _():
        with jax.named_scope("leg1"):
            leg1_arrived()
        leg2().start()

    for a in range(2, HOPS + 1, 2):
        ring_range(a, min(a + 2, HOPS + 1))

    def spreads(early):
        for e in range(SIDE):
            for k in range(2):
                for d in order:
                    a, b = (e, d) if k == 0 else (d, e)
                    c = lax.rem(x + SIDE - a, SIDE) * SIDE + lax.rem(y + SIDE - b, SIDE)
                    m = row_of(c)

                    @pl.when(both((comes_at(m) <= EARLY) == early, second_goes(m, col)))
                    def _():
                        second(k, e, d, m).wait_recv()

    def pairs(s, carry):
        for h in range(CUTS):
            for direction in range(2):
                m = origin(direction, s)

                @pl.when(both(travels(m, direction, s, h), wanted(m)))
                def _():
                    to_pair(direction, s, h, m).wait_recv()

        return carry

    def add(m):
        left = tp[m]
        right = panel[pl.ds(2 * m, 2)].reshape(2 * wr, wc)
        g_ref[...] += lax.dot_general(left, right, (((0,), (0,)), ((), ())), preferred_element_type=F32)

    with jax.named_scope("pairs"):
        spreads(True)
        for k in range(2):
            own_pair(k).wait_recv()
        lax.fori_loop(1, EARLY + 1, pairs, 0)

    def add_blocks(early):
        def step(m, carry):
            @pl.when(both(wanted(m), (comes_at(m) <= EARLY) == early))
            def _():
                add(m)

            return carry

        lax.fori_loop(0, N, step, 0)

    with jax.named_scope("gram"):
        add_blocks(True)

    with jax.named_scope("last"):
        spreads(False)
        lax.fori_loop(EARLY + 1, HOPS + 1, pairs, 0)
        add_blocks(False)
        for direction in range(2):
            for s in range(1, FAR + 1 - direction):
                u_pair(direction, s, origin(direction, s)).wait_recv()
    gb[...] = jnp.transpose(g_ref[...].astype(BF16))

    lanes = wr // 2

    def half_of(k):
        return pl.ds(k * lanes, lanes)

    def line(ref, k, i):
        return ref.at[i, :, :, half_of(k)] if k == 0 else ref.at[:, i, :, half_of(k)]

    def place(k, d):
        return lax.rem((y if k else x) + d, SIDE)

    def reduce1(k, d):
        return copy(
            line(part, k, place(k, d)), row_in.at[k, d - 1], r1_send.at[k, d - 1], r1_recv.at[k, d - 1],
            row, moved(k, d),
        )

    def reduce2(k, d):
        return copy(
            mids.at[k, place(1 - k, d)], last_in.at[k, d - 1], r2_send.at[k, d - 1], r2_recv.at[k, d - 1],
            row, moved(1 - k, d),
        )

    def child_part(i, carry):
        cpl = upanel[pl.ds(2 * SIDE * i, 2 * SIDE)].reshape(SIDE * part.shape[2], wc)
        prod = jnp.dot(cpl, gb[...], preferred_element_type=F32).astype(BF16)
        part[i] = prod.reshape(SIDE, *part.shape[2:])
        return carry

    with jax.named_scope("child"):
        lax.fori_loop(0, SIDE, child_part, 0)
    for d in order:
        for k in range(2):
            reduce1(k, d).start()

    def sent(s, carry):
        for direction in range(2):
            m = origin(direction, s - 1)
            got = origin(direction, s)
            for h in range(CUTS):
                @pl.when(travels(m, direction, s, h))
                def _():
                    hop(direction, s, h, m, False).wait_send()

                @pl.when(both(travels(got, direction, s, h), wanted(got)))
                def _():
                    to_pair(direction, s, h, got).wait_send()

            @pl.when(s < FAR + 1 - direction)
            def _():
                u_hop(direction, s, m, False).wait_send()
                u_pair(direction, s, got).wait_send()

        return carry

    with jax.named_scope("sends"):
        lax.fori_loop(1, HOPS + 1, sent, 0)
        for k in range(2):
            own_pair(k).wait_send()

            @pl.when(both(mirrors(z, col), jnp.logical_not(stays(k, z))))
            def _():
                leg1(k, stage.at[my_rows]).wait_send()

            for e in range(SIDE):
                second_all(k, e, row_of(moved(k, SIDE - e if e else 0)), lambda c: c.wait_send())

        first_all(lambda c: c.wait_send())

        @pl.when(mirrors(z, turn))
        def _():
            leg2().wait_send()

        def handed(h, m, sem_of):
            for k in range(2):
                @pl.when(jnp.logical_not(stays(k, m)))
                def _():
                    hand(k, h, m, w_ref.at[rows_of(h)], sem_of(k)).wait_send()

        @pl.when(col == z)
        def _():
            for h in range(CUTS):
                handed(h, z, lambda k: hand_own.at[h, k])

            def handed_on(s, carry):
                for h in range(CUTS):
                    for direction in range(2):
                        m = origin(direction, s)

                        @pl.when(both(travels(m, direction, s, h), m >= z))
                        def _():
                            handed(h, m, lambda k: hand_send.at[direction, s - 1, h, k])

                return carry

            lax.fori_loop(1, NEAR + 1, handed_on, 0)

    with jax.named_scope("reduce1"):
        for k in range(2):
            mine = part[x, :, :, half_of(k)] if k == 0 else part[:, y, :, half_of(k)]
            sums[k] = mine.astype(F32)
            for d in order:
                reduce1(k, d).wait_recv()
                sums[k] += row_in[k, d - 1].astype(F32)
            mids[k] = sums[k].astype(BF16)
            for d in order:
                reduce2(k, d).start()
    with jax.named_scope("reduce2"):
        for k in range(2):
            total = sums[k, y if k == 0 else x]
            for d in order:
                reduce2(k, d).wait_recv()
                total += last_in[k, d - 1].astype(F32)
            child_ref[:, half_of(k)] = jnp.where(member_ref[:, half_of(k)] > 0, -total, 0.0)
        for k in range(2):
            for d in order:
                reduce1(k, d).wait_send()
                reduce2(k, d).wait_send()


def body(factor, sel_tiles, coupling):
    rows, cols = lax.axis_size("row"), lax.axis_size("col")
    assert rows == 2 * N and cols == N
    wr, wc = factor.shape
    kc = coupling.shape[1]
    row_index = lax.axis_index("row")
    kb = rows * kc // cols
    dma = pltpu.SemaphoreType.DMA
    vm = pl.BlockSpec(memory_space=pltpu.VMEM)
    global_rows = row_index * wr + jnp.arange(wr, dtype=jnp.int32)
    member = jnp.any((global_rows // TILE)[:, None] == sel_tiles[None, :], axis=1)
    pair_of = lambda *shape: [dma(shape), dma(shape)]
    gram, child = pl.pallas_call(
        kernel,
        out_shape=(
            jax.ShapeDtypeStruct((wr, wc), F32),
            jax.ShapeDtypeStruct((kb, wr), F32),
        ),
        in_specs=[vm, vm, vm],
        out_specs=(vm, vm),
        scratch_shapes=[
            pltpu.VMEM((rows, wr, wc), BF16),
            pltpu.VMEM((rows, kc, wc), BF16),
            pltpu.VMEM((cols, 2 * wr, wc // 2), BF16),
            pltpu.VMEM((2 * wr, wc // 2), BF16),
            pltpu.VMEM((wc, wr), BF16),
            pltpu.VMEM((SIDE, SIDE, kb, wr), BF16),
            pltpu.VMEM((2, SIDE, kb, wr // 2), F32),
            pltpu.VMEM((2, SIDE, kb, wr // 2), BF16),
            pltpu.VMEM((2, SIDE - 1, SIDE, kb, wr // 2), BF16),
            pltpu.VMEM((2, SIDE - 1, kb, wr // 2), BF16),
            *pair_of(2, HOPS, CUTS), *pair_of(2, FAR), *pair_of(2, HOPS, CUTS), *pair_of(2, FAR),
            *pair_of(2),
            *pair_of(2), dma, dma, dma((2, NEAR, CUTS, 2)), dma((2, CUTS)), dma((CUTS, 2)),
            *pair_of(2, SIDE - 1), *pair_of(2, SIDE, SIDE - 1), *pair_of(2, SIDE - 1), *pair_of(2, SIDE - 1),
        ],
        compiler_params=pltpu.CompilerParams(
            collective_id=0, has_side_effects=True, vmem_limit_bytes=52 * 2**20
        ),
    )(factor, coupling.T, member.astype(F32)[None, :])
    return gram, child


def solution(mesh):
    return jax.shard_map(
        body,
        mesh=mesh,
        in_specs=(P("row", "col"), P(), P("col", "row")),
        out_specs=(P("row", "col"), P("col", "row")),
        check_vma=False,
    )
```

```python
import jax
import jax.numpy as jnp
from jax import lax
from jax.experimental import pallas as pl
from jax.experimental.pallas import tpu as pltpu
from jax.sharding import PartitionSpec as P

TILE = 128
MESH = pl.DeviceIdType.MESH
F32 = jnp.float32
BF16 = jnp.bfloat16
SIDE = 4
N = SIDE * SIDE
FAR = N // 2
CUTS = 2
HOPS = FAR
NEAR = (6, 4)
MIRRORED = 4
EARLY = 5


def both(*conditions):
    out = conditions[0]
    for c in conditions[1:]:
        out = jnp.logical_and(out, c)
    return out


def kernel(
    w_ref, ut_ref, member_ref, g_ref, child_ref,
    panel, upanel, tp, stage, gb, part, sums, mids, row_in, last_in,
    ring_send, ring_recv, u_send, u_recv, pair_send, pair_recv, upair_send, upair_recv,
    own_send, own_recv,
    leg1_send, leg1_recv, leg2_send, leg2_recv, hand_send, hand_recv, hand_own,
    p1_send, p1_recv, p2_send, p2_recv, r1_send, r1_recv, r2_send, r2_recv,
):
    row = lax.axis_index("row")
    col = lax.axis_index("col")
    rows = 2 * N
    core = lax.rem(row, 2)
    z = row // 2
    x = col // SIDE
    y = lax.rem(col, SIDE)
    other = 1 - core
    partner = 2 * z + other
    up = lax.rem(row + 2, rows)
    down = lax.rem(row + rows - 2, rows)
    wr, wc = w_ref.shape
    half = wc // 2
    chunk = wr // CUTS

    def copy(src, dst, ssem, rsem, r, c):
        return pltpu.make_async_remote_copy(
            src_ref=src, dst_ref=dst, send_sem=ssem, recv_sem=rsem,
            device_id=(r, c), device_id_type=MESH,
        )

    def travels(m, direction, s, h):
        near = jnp.logical_or(s < FAR, h % 2 == direction)
        return both(m >= col, m >= FAR if direction == 0 else s <= m, near)

    def gap(m, plane):
        return jnp.where(m - plane <= FAR, m - plane, N - (m - plane))

    def comes_at(m):
        return gap(m, z)

    def wanted(m):
        return both(m >= col, m >= z)

    def origin(direction, s):
        return lax.rem(z + (N - s if direction == 0 else s), N)

    barrier = pltpu.get_barrier_semaphore()

    def greet(r, c):
        pl.semaphore_signal(barrier, inc=1, device_id=(r, c), device_id_type=MESH)

    turn = lax.rem(col + 2 * N - z - FAR * core, N)
    for r in (up, down, partner):
        greet(r, col)
    for d in range(1, N):
        greet(row, lax.rem(col + d, N))
    greet(partner, turn)

    @pl.when(turn != z)
    def _():
        greet(2 * turn + core, col)

    @pl.when(col != z)
    def _():
        greet(partner, z)

    with jax.named_scope("barrier"):
        pl.semaphore_wait(barrier, N + 3 + jnp.where(turn != z, 1, 0) + jnp.where(col == z, N - 1, 0))

    def rows_of(h):
        return pl.ds(h * chunk, chunk)

    def towards(direction):
        return up if direction == 0 else down

    def slot_of(m):
        return 2 * m + core

    def hop(direction, s, h, m, first):
        dst = panel.at[slot_of(m), rows_of(h)]
        return copy(
            w_ref.at[rows_of(h)] if first else dst, dst,
            ring_send.at[direction, s - 1, h], ring_recv.at[direction, s - 1, h], towards(direction), col,
        )

    def u_hop(direction, s, m, first):
        dst = upanel.at[slot_of(m)]
        return copy(
            ut_ref if first else dst, dst, u_send.at[direction, s - 1], u_recv.at[direction, s - 1],
            towards(direction), col,
        )

    def to_pair(direction, s, h, m):
        ref = panel.at[slot_of(m), rows_of(h)]
        return copy(
            ref, ref, pair_send.at[direction, s - 1, h], pair_recv.at[direction, s - 1, h], partner, col
        )

    def u_pair(direction, s, m):
        ref = upanel.at[slot_of(m)]
        return copy(ref, ref, upair_send.at[direction, s - 1], upair_recv.at[direction, s - 1], partner, col)

    def own_pair(k):
        src, dst = ((w_ref, panel), (ut_ref, upanel))[k]
        return copy(src, dst.at[row], own_send.at[k], own_recv.at[k], partner, col)

    def part_rows(k):
        return pl.ds(k * wr, wr)

    my_rows = pl.ds(pl.multiple_of(core * wr, wr), wr)

    def leg1(k, dst):
        to = lax.rem(z + col + FAR * k, N)
        return copy(
            w_ref.at[:, pl.ds(k * half, half)], dst, leg1_send.at[k], leg1_recv.at[core], 2 * z + k, to
        )

    def stays(k, m):
        return both(core == k, lax.rem(m + FAR * k, N) == 0)

    def mirrors(m, plane):
        return both(m - plane > NEAR[1], N - (m - plane) > NEAR[0])

    def leg2():
        return copy(stage, tp.at[z], leg2_send, leg2_recv, 2 * turn + core, col)

    for h in range(CUTS):
        for direction in range(2):
            @pl.when(travels(z, direction, 1, h))
            def _():
                hop(direction, 1, h, z, True).start()

    for k in range(2):
        @pl.when(both(mirrors(z, col), jnp.logical_not(stays(k, z))))
        def _():
            leg1(k, stage.at[my_rows]).start()

        @pl.when(both(mirrors(z, col), stays(k, z)))
        def _():
            stage[my_rows] = w_ref[:, pl.ds(k * half, half)]

    def hand(k, h, m, src, sem):
        return copy(
            src.at[:, pl.ds(k * half, half)],
            tp.at[m, pl.ds(pl.multiple_of(core * wr + h * chunk, chunk), chunk)],
            sem, hand_recv.at[core, h], 2 * z + k, lax.rem(m + z + FAR * k, N),
        )

    def hands(h, m, src, sem_of):
        for k in range(2):
            @pl.when(stays(k, m))
            def _():
                tp[m, pl.ds(pl.multiple_of(core * wr + h * chunk, chunk), chunk)] = src[:, pl.ds(k * half, half)]

            @pl.when(jnp.logical_not(stays(k, m)))
            def _():
                hand(k, h, m, src, sem_of(k)).start()

    @pl.when(col == z)
    def _():
        for h in range(CUTS):
            hands(h, z, w_ref.at[rows_of(h)], lambda k: hand_own.at[h, k])

    for direction in range(2):
        u_hop(direction, 1, z, True).start()
    for k in range(2):
        own_pair(k).start()
    panel[row] = w_ref[...]
    upanel[row] = ut_ref[...]
    g_ref[...] = jnp.zeros_like(g_ref)

    def leg1_arrived():
        for k in range(2):
            @pl.when(jnp.logical_not(both(turn == col, core == k)))
            def _():
                copy(
                    w_ref.at[:, pl.ds(0, half)], stage.at[part_rows(k)], leg1_send.at[k], leg1_recv.at[k],
                    row, col,
                ).wait_recv()

    def moved(k, d):
        if k == 0:
            return lax.rem(x + d, SIDE) * SIDE + y
        return x * SIDE + lax.rem(y + d, SIDE)

    def row_of(c):
        return lax.rem(c + 2 * N - z - FAR * core, N)

    def least(k, c):
        return c // SIDE * SIDE if k == 0 else lax.rem(c, SIDE)

    def first(k, d, m):
        ref = tp.at[m, part_rows(k)]
        return copy(ref, ref, p1_send.at[k, d - 1], p1_recv.at[k, d - 1], row, moved(k, d))

    def second(k, e, d, m):
        ref = tp.at[m, part_rows(k)]
        return copy(ref, ref, p2_send.at[k, e, d - 1], p2_recv.at[k, e, d - 1], row, moved(1 - k, d))

    def first_goes(k, m, c):
        return both(m >= z, m >= least(k, c))

    def second_goes(m, c):
        return both(m >= z, m >= c)

    order = (1, 3, 2)
    mine = turn

    def first_all(action):
        for d in order:
            for k in range(2):
                @pl.when(first_goes(k, mine, moved(k, d)))
                def _():
                    action(first(k, d, mine))

    def second_all(k, e, m, action):
        for d in order:
            @pl.when(second_goes(m, moved(1 - k, d)))
            def _():
                action(second(k, e, d, m))

    def starts_at(m):
        return jnp.where(mirrors(m, z), MIRRORED, comes_at(m) + 1)

    def spread(s):
        @pl.when(both(mine >= z, starts_at(mine) == s))
        def _():
            @pl.when(mirrors(mine, z))
            def _():
                copy(stage, tp.at[mine], leg2_send, leg2_recv, row, col).wait_recv()

            for k in range(2):
                @pl.when(jnp.logical_not(jnp.logical_or(mirrors(mine, z), both(col == z, core == k))))
                def _():
                    for h in range(CUTS):
                        pltpu.make_async_remote_copy(
                            src_ref=w_ref.at[rows_of(h), pl.ds(0, half)],
                            dst_ref=tp.at[mine, pl.ds(k * wr + h * chunk, chunk)],
                            send_sem=hand_own.at[h, k], recv_sem=hand_recv.at[k, h],
                            device_id=(partner, col), device_id_type=MESH,
                        ).wait_recv()

            first_all(lambda c: c.start())
            for k in range(2):
                second_all(k, 0, mine, lambda c: c.start())

    def relay(s):
        for e in order:
            for k in range(2):
                m = row_of(moved(k, SIDE - e))

                @pl.when(both(starts_at(m) + 1 == s, first_goes(k, m, col)))
                def _():
                    first(k, e, m).wait_recv()
                    second_all(k, e, m, lambda c: c.start())

    def passes(s):
        for h in range(CUTS):
            for direction in range(2):
                m = origin(direction, s)

                @pl.when(travels(m, direction, s, h))
                def _():
                    hop(direction, s, h, m, False).wait_recv()

                    @pl.when(both(s < HOPS, travels(m, direction, s + 1, h)))
                    def _():
                        hop(direction, s + 1, h, m, False).start()

                    @pl.when(wanted(m))
                    def _():
                        to_pair(direction, s, h, m).start()

                    @pl.when(both(col == z, m >= z, s <= NEAR[direction]))
                    def _():
                        src = panel.at[slot_of(m), rows_of(h)]
                        hands(h, m, src, lambda k: hand_send.at[direction, s - 1, h, k])

    def u_passes(s):
        for direction in range(2):
            m = origin(direction, s)

            @pl.when(both(s >= 1, s < FAR + 1 - direction))
            def _():
                u_hop(direction, s, m, False).wait_recv()

                @pl.when(s < FAR - direction)
                def _():
                    u_hop(direction, s + 1, m, False).start()

                u_pair(direction, s, m).start()

    def ring_step(s, carry):
        passes(s)
        u_passes(s - 1)
        spread(s)
        relay(s)
        return carry

    def ring_range(a, b):
        with jax.named_scope("ring%d" % a):
            lax.fori_loop(a, b, ring_step, 0)

    ring_range(1, 2)

    @pl.when(mirrors(z, turn))
    def _():
        with jax.named_scope("leg1"):
            leg1_arrived()
        leg2().start()

    for a in range(2, HOPS + 1, 2):
        ring_range(a, min(a + 2, HOPS + 1))

    def spreads(early):
        for e in range(SIDE):
            for k in range(2):
                for d in order:
                    a, b = (e, d) if k == 0 else (d, e)
                    c = lax.rem(x + SIDE - a, SIDE) * SIDE + lax.rem(y + SIDE - b, SIDE)
                    m = row_of(c)

                    @pl.when(both((comes_at(m) <= EARLY) == early, second_goes(m, col)))
                    def _():
                        second(k, e, d, m).wait_recv()

    def pairs(s, carry):
        for h in range(CUTS):
            for direction in range(2):
                m = origin(direction, s)

                @pl.when(both(travels(m, direction, s, h), wanted(m)))
                def _():
                    to_pair(direction, s, h, m).wait_recv()

        return carry

    def add(m):
        left = tp[m]
        right = panel[pl.ds(2 * m, 2)].reshape(2 * wr, wc)
        g_ref[...] += lax.dot_general(left, right, (((0,), (0,)), ((), ())), preferred_element_type=F32)

    u_passes(HOPS)
    with jax.named_scope("pairs"):
        spreads(True)
        for k in range(2):
            own_pair(k).wait_recv()
        lax.fori_loop(1, EARLY + 1, pairs, 0)

    def add_blocks(early):
        def step(m, carry):
            @pl.when(both(wanted(m), (comes_at(m) <= EARLY) == early))
            def _():
                add(m)

            return carry

        lax.fori_loop(0, N, step, 0)

    with jax.named_scope("gram"):
        add_blocks(True)

    with jax.named_scope("last"):
        spreads(False)
        lax.fori_loop(EARLY + 1, HOPS + 1, pairs, 0)
        add_blocks(False)
        for direction in range(2):
            for s in range(1, FAR + 1 - direction):
                u_pair(direction, s, origin(direction, s)).wait_recv()
    gb[...] = jnp.transpose(g_ref[...].astype(BF16))

    lanes = wr // 2

    def half_of(k):
        return pl.ds(k * lanes, lanes)

    def line(ref, k, i):
        return ref.at[i, :, :, half_of(k)] if k == 0 else ref.at[:, i, :, half_of(k)]

    def place(k, d):
        return lax.rem((y if k else x) + d, SIDE)

    def reduce1(k, d):
        return copy(
            line(part, k, place(k, d)), row_in.at[k, d - 1], r1_send.at[k, d - 1], r1_recv.at[k, d - 1],
            row, moved(k, d),
        )

    def reduce2(k, d):
        return copy(
            mids.at[k, place(1 - k, d)], last_in.at[k, d - 1], r2_send.at[k, d - 1], r2_recv.at[k, d - 1],
            row, moved(1 - k, d),
        )

    def child_part(i, carry):
        cpl = upanel[pl.ds(2 * SIDE * i, 2 * SIDE)].reshape(SIDE * part.shape[2], wc)
        prod = jnp.dot(cpl, gb[...], preferred_element_type=F32).astype(BF16)
        part[i] = prod.reshape(SIDE, *part.shape[2:])
        return carry

    with jax.named_scope("child"):
        lax.fori_loop(0, SIDE, child_part, 0)
    for d in order:
        for k in range(2):
            reduce1(k, d).start()

    def sent(s, carry):
        for direction in range(2):
            m = origin(direction, s - 1)
            got = origin(direction, s)
            for h in range(CUTS):
                @pl.when(travels(m, direction, s, h))
                def _():
                    hop(direction, s, h, m, False).wait_send()

                @pl.when(both(travels(got, direction, s, h), wanted(got)))
                def _():
                    to_pair(direction, s, h, got).wait_send()

            @pl.when(s < FAR + 1 - direction)
            def _():
                u_hop(direction, s, m, False).wait_send()
                u_pair(direction, s, got).wait_send()

        return carry

    with jax.named_scope("sends"):
        lax.fori_loop(1, HOPS + 1, sent, 0)
        for k in range(2):
            own_pair(k).wait_send()

            @pl.when(both(mirrors(z, col), jnp.logical_not(stays(k, z))))
            def _():
                leg1(k, stage.at[my_rows]).wait_send()

            for e in range(SIDE):
                second_all(k, e, row_of(moved(k, SIDE - e if e else 0)), lambda c: c.wait_send())

        first_all(lambda c: c.wait_send())

        @pl.when(mirrors(z, turn))
        def _():
            leg2().wait_send()

        def handed(h, m, sem_of):
            for k in range(2):
                @pl.when(jnp.logical_not(stays(k, m)))
                def _():
                    hand(k, h, m, w_ref.at[rows_of(h)], sem_of(k)).wait_send()

        @pl.when(col == z)
        def _():
            for h in range(CUTS):
                handed(h, z, lambda k: hand_own.at[h, k])

            def handed_on(s, carry):
                for h in range(CUTS):
                    for direction in range(2):
                        m = origin(direction, s)

                        @pl.when(both(travels(m, direction, s, h), m >= z, s <= NEAR[direction]))
                        def _():
                            handed(h, m, lambda k: hand_send.at[direction, s - 1, h, k])

                return carry

            lax.fori_loop(1, max(NEAR) + 1, handed_on, 0)

    with jax.named_scope("reduce1"):
        for k in range(2):
            mine = part[x, :, :, half_of(k)] if k == 0 else part[:, y, :, half_of(k)]
            sums[k] = mine.astype(F32)
            for d in order:
                reduce1(k, d).wait_recv()
                sums[k] += row_in[k, d - 1].astype(F32)
            mids[k] = sums[k].astype(BF16)
            for d in order:
                reduce2(k, d).start()
    with jax.named_scope("reduce2"):
        for k in range(2):
            total = sums[k, y if k == 0 else x]
            for d in order:
                reduce2(k, d).wait_recv()
                total += last_in[k, d - 1].astype(F32)
            child_ref[:, half_of(k)] = jnp.where(member_ref[:, half_of(k)] > 0, -total, 0.0)
        for k in range(2):
            for d in order:
                reduce1(k, d).wait_send()
                reduce2(k, d).wait_send()


def body(factor, sel_tiles, coupling):
    rows, cols = lax.axis_size("row"), lax.axis_size("col")
    assert rows == 2 * N and cols == N
    wr, wc = factor.shape
    kc = coupling.shape[1]
    row_index = lax.axis_index("row")
    kb = rows * kc // cols
    dma = pltpu.SemaphoreType.DMA
    vm = pl.BlockSpec(memory_space=pltpu.VMEM)
    global_rows = row_index * wr + jnp.arange(wr, dtype=jnp.int32)
    member = jnp.any((global_rows // TILE)[:, None] == sel_tiles[None, :], axis=1)
    pair_of = lambda *shape: [dma(shape), dma(shape)]
    gram, child = pl.pallas_call(
        kernel,
        out_shape=(
            jax.ShapeDtypeStruct((wr, wc), F32),
            jax.ShapeDtypeStruct((kb, wr), F32),
        ),
        in_specs=[vm, vm, vm],
        out_specs=(vm, vm),
        scratch_shapes=[
            pltpu.VMEM((rows, wr, wc), BF16),
            pltpu.VMEM((rows, kc, wc), BF16),
            pltpu.VMEM((cols, 2 * wr, wc // 2), BF16),
            pltpu.VMEM((2 * wr, wc // 2), BF16),
            pltpu.VMEM((wc, wr), BF16),
            pltpu.VMEM((SIDE, SIDE, kb, wr), BF16),
            pltpu.VMEM((2, SIDE, kb, wr // 2), F32),
            pltpu.VMEM((2, SIDE, kb, wr // 2), BF16),
            pltpu.VMEM((2, SIDE - 1, SIDE, kb, wr // 2), BF16),
            pltpu.VMEM((2, SIDE - 1, kb, wr // 2), BF16),
            *pair_of(2, HOPS, CUTS), *pair_of(2, FAR), *pair_of(2, HOPS, CUTS), *pair_of(2, FAR),
            *pair_of(2),
            *pair_of(2), dma, dma, dma((2, max(NEAR), CUTS, 2)), dma((2, CUTS)), dma((CUTS, 2)),
            *pair_of(2, SIDE - 1), *pair_of(2, SIDE, SIDE - 1), *pair_of(2, SIDE - 1), *pair_of(2, SIDE - 1),
        ],
        compiler_params=pltpu.CompilerParams(
            collective_id=0, has_side_effects=True, vmem_limit_bytes=52 * 2**20
        ),
    )(factor, coupling.T, member.astype(F32)[None, :])
    return gram, child


def solution(mesh):
    return jax.shard_map(
        body,
        mesh=mesh,
        in_specs=(P("row", "col"), P(), P("col", "row")),
        out_specs=(P("row", "col"), P("col", "row")),
        check_vma=False,
    )
```

```python
import jax
import jax.numpy as jnp
from jax import lax
from jax.experimental import pallas as pl
from jax.experimental.pallas import tpu as pltpu
from jax.sharding import PartitionSpec as P

TILE = 128
MESH = pl.DeviceIdType.MESH
F32 = jnp.float32
BF16 = jnp.bfloat16
SIDE = 4
N = SIDE * SIDE
FAR = N // 2
SHIFT = 9
CUTS = 2
HOPS = FAR
NEAR = (6, 4)
MIRRORED = 4
EARLY = 4


def both(*conditions):
    out = conditions[0]
    for c in conditions[1:]:
        out = jnp.logical_and(out, c)
    return out


def kernel(
    w_ref, ut_ref, member_ref, g_ref, child_ref,
    panel, upanel, tp, stage, gb, part, sums, mids, row_in, last_in,
    ring_send, ring_recv, u_send, u_recv, pair_send, pair_recv, upair_send, upair_recv,
    own_send, own_recv,
    leg1_send, leg1_recv, leg2_send, leg2_recv, hand_send, hand_recv, hand_own,
    p1_send, p1_recv, p2_send, p2_recv, r1_send, r1_recv, r2_send, r2_recv,
):
    row = lax.axis_index("row")
    col = lax.axis_index("col")
    rows = 2 * N
    core = lax.rem(row, 2)
    z = row // 2
    x = col // SIDE
    y = lax.rem(col, SIDE)
    other = 1 - core
    partner = 2 * z + other
    up = lax.rem(row + 2, rows)
    down = lax.rem(row + rows - 2, rows)
    wr, wc = w_ref.shape
    half = wc // 2
    chunk = wr // CUTS

    def copy(src, dst, ssem, rsem, r, c):
        return pltpu.make_async_remote_copy(
            src_ref=src, dst_ref=dst, send_sem=ssem, recv_sem=rsem,
            device_id=(r, c), device_id_type=MESH,
        )

    def travels(m, direction, s, h):
        near = jnp.logical_or(s < FAR, h % 2 == direction)
        return both(m >= col, m >= FAR if direction == 0 else s <= m, near)

    def gap(m, plane):
        return jnp.where(m - plane <= FAR, m - plane, N - (m - plane))

    def comes_at(m):
        return gap(m, z)

    def wanted(m):
        return both(m >= col, m >= z)

    def origin(direction, s):
        return lax.rem(z + (N - s if direction == 0 else s), N)

    barrier = pltpu.get_barrier_semaphore()

    def greet(r, c):
        pl.semaphore_signal(barrier, inc=1, device_id=(r, c), device_id_type=MESH)

    turn = lax.rem(col + 2 * N - z - SHIFT * core, N)
    for r in (up, down, partner):
        greet(r, col)
    for d in range(1, N):
        greet(row, lax.rem(col + d, N))
    greet(partner, turn)

    @pl.when(turn != z)
    def _():
        greet(2 * turn + core, col)

    @pl.when(col != z)
    def _():
        greet(partner, z)

    with jax.named_scope("barrier"):
        pl.semaphore_wait(barrier, N + 3 + jnp.where(turn != z, 1, 0) + jnp.where(col == z, N - 1, 0))

    def rows_of(h):
        return pl.ds(h * chunk, chunk)

    def towards(direction):
        return up if direction == 0 else down

    def slot_of(m):
        return 2 * m + core

    def hop(direction, s, h, m, first):
        dst = panel.at[slot_of(m), rows_of(h)]
        return copy(
            w_ref.at[rows_of(h)] if first else dst, dst,
            ring_send.at[direction, s - 1, h], ring_recv.at[direction, s - 1, h], towards(direction), col,
        )

    def u_hop(direction, s, m, first):
        dst = upanel.at[slot_of(m)]
        return copy(
            ut_ref if first else dst, dst, u_send.at[direction, s - 1], u_recv.at[direction, s - 1],
            towards(direction), col,
        )

    def to_pair(direction, s, h, m):
        ref = panel.at[slot_of(m), rows_of(h)]
        return copy(
            ref, ref, pair_send.at[direction, s - 1, h], pair_recv.at[direction, s - 1, h], partner, col
        )

    def u_pair(direction, s, m):
        ref = upanel.at[slot_of(m)]
        return copy(ref, ref, upair_send.at[direction, s - 1], upair_recv.at[direction, s - 1], partner, col)

    def own_pair(k):
        src, dst = ((w_ref, panel), (ut_ref, upanel))[k]
        return copy(src, dst.at[row], own_send.at[k], own_recv.at[k], partner, col)

    def part_rows(k):
        return pl.ds(k * wr, wr)

    my_rows = pl.ds(pl.multiple_of(core * wr, wr), wr)

    def leg1(k, dst):
        to = lax.rem(z + col + SHIFT * k, N)
        return copy(
            w_ref.at[:, pl.ds(k * half, half)], dst, leg1_send.at[k], leg1_recv.at[core], 2 * z + k, to
        )

    def stays(k, m):
        return both(core == k, lax.rem(m + SHIFT * k, N) == 0)

    def mirrors(m, plane):
        return both(m - plane > NEAR[1], N - (m - plane) > NEAR[0])

    def leg2():
        return copy(stage, tp.at[z], leg2_send, leg2_recv, 2 * turn + core, col)

    for h in range(CUTS):
        for direction in range(2):
            @pl.when(travels(z, direction, 1, h))
            def _():
                hop(direction, 1, h, z, True).start()

    for k in range(2):
        @pl.when(both(mirrors(z, col), jnp.logical_not(stays(k, z))))
        def _():
            leg1(k, stage.at[my_rows]).start()

        @pl.when(both(mirrors(z, col), stays(k, z)))
        def _():
            stage[my_rows] = w_ref[:, pl.ds(k * half, half)]

    def hand(k, h, m, src, sem):
        return copy(
            src.at[:, pl.ds(k * half, half)],
            tp.at[m, pl.ds(pl.multiple_of(core * wr + h * chunk, chunk), chunk)],
            sem, hand_recv.at[core, h], 2 * z + k, lax.rem(m + z + SHIFT * k, N),
        )

    def hands(h, m, src, sem_of):
        for k in range(2):
            @pl.when(stays(k, m))
            def _():
                tp[m, pl.ds(pl.multiple_of(core * wr + h * chunk, chunk), chunk)] = src[:, pl.ds(k * half, half)]

            @pl.when(jnp.logical_not(stays(k, m)))
            def _():
                hand(k, h, m, src, sem_of(k)).start()

    @pl.when(col == z)
    def _():
        for h in range(CUTS):
            hands(h, z, w_ref.at[rows_of(h)], lambda k: hand_own.at[h, k])

    for direction in range(2):
        u_hop(direction, 1, z, True).start()
    for k in range(2):
        own_pair(k).start()
    panel[row] = w_ref[...]
    upanel[row] = ut_ref[...]
    g_ref[...] = jnp.zeros_like(g_ref)

    def leg1_arrived():
        for k in range(2):
            @pl.when(jnp.logical_not(both(turn == col, core == k)))
            def _():
                copy(
                    w_ref.at[:, pl.ds(0, half)], stage.at[part_rows(k)], leg1_send.at[k], leg1_recv.at[k],
                    row, col,
                ).wait_recv()

    def moved(k, d):
        if k == 0:
            return lax.rem(x + d, SIDE) * SIDE + y
        return x * SIDE + lax.rem(y + d, SIDE)

    def row_of(c):
        return lax.rem(c + 2 * N - z - SHIFT * core, N)

    def least(k, c):
        return c // SIDE * SIDE if k == 0 else lax.rem(c, SIDE)

    def first(k, d, m):
        ref = tp.at[m, part_rows(k)]
        return copy(ref, ref, p1_send.at[k, d - 1], p1_recv.at[k, d - 1], row, moved(k, d))

    def second(k, e, d, m):
        ref = tp.at[m, part_rows(k)]
        return copy(ref, ref, p2_send.at[k, e, d - 1], p2_recv.at[k, e, d - 1], row, moved(1 - k, d))

    def first_goes(k, m, c):
        return both(m >= z, m >= least(k, c))

    def second_goes(m, c):
        return both(m >= z, m >= c)

    order = (1, 3, 2)
    mine = turn

    def first_all(action):
        for d in order:
            for k in range(2):
                @pl.when(first_goes(k, mine, moved(k, d)))
                def _():
                    action(first(k, d, mine))

    def second_all(k, e, m, action):
        for d in order:
            @pl.when(second_goes(m, moved(1 - k, d)))
            def _():
                action(second(k, e, d, m))

    def starts_at(m):
        return jnp.where(mirrors(m, z), MIRRORED, comes_at(m) + 1)

    def spread(s):
        @pl.when(both(mine >= z, starts_at(mine) == s))
        def _():
            @pl.when(mirrors(mine, z))
            def _():
                copy(stage, tp.at[mine], leg2_send, leg2_recv, row, col).wait_recv()

            for k in range(2):
                @pl.when(jnp.logical_not(jnp.logical_or(mirrors(mine, z), both(col == z, core == k))))
                def _():
                    for h in range(CUTS):
                        pltpu.make_async_remote_copy(
                            src_ref=w_ref.at[rows_of(h), pl.ds(0, half)],
                            dst_ref=tp.at[mine, pl.ds(k * wr + h * chunk, chunk)],
                            send_sem=hand_own.at[h, k], recv_sem=hand_recv.at[k, h],
                            device_id=(partner, col), device_id_type=MESH,
                        ).wait_recv()

            first_all(lambda c: c.start())
            for k in range(2):
                second_all(k, 0, mine, lambda c: c.start())

    def relay(s):
        for e in order:
            for k in range(2):
                m = row_of(moved(k, SIDE - e))

                @pl.when(both(starts_at(m) + 1 == s, first_goes(k, m, col)))
                def _():
                    first(k, e, m).wait_recv()
                    second_all(k, e, m, lambda c: c.start())

    def passes(s):
        for h in range(CUTS):
            for direction in range(2):
                m = origin(direction, s)

                @pl.when(travels(m, direction, s, h))
                def _():
                    hop(direction, s, h, m, False).wait_recv()

                    @pl.when(both(s < HOPS, travels(m, direction, s + 1, h)))
                    def _():
                        hop(direction, s + 1, h, m, False).start()

                    @pl.when(wanted(m))
                    def _():
                        to_pair(direction, s, h, m).start()

                    @pl.when(both(col == z, m >= z, s <= NEAR[direction]))
                    def _():
                        src = panel.at[slot_of(m), rows_of(h)]
                        hands(h, m, src, lambda k: hand_send.at[direction, s - 1, h, k])

    def u_passes(s):
        for direction in range(2):
            m = origin(direction, s)

            @pl.when(both(s >= 1, s < FAR + 1 - direction))
            def _():
                u_hop(direction, s, m, False).wait_recv()

                @pl.when(s < FAR - direction)
                def _():
                    u_hop(direction, s + 1, m, False).start()

                u_pair(direction, s, m).start()

    def ring_step(s, carry):
        passes(s)
        u_passes(s - 1)
        spread(s)
        relay(s)
        return carry

    def ring_range(a, b):
        with jax.named_scope("ring%d" % a):
            lax.fori_loop(a, b, ring_step, 0)

    ring_range(1, 2)

    @pl.when(mirrors(z, turn))
    def _():
        with jax.named_scope("leg1"):
            leg1_arrived()
        leg2().start()

    for a in range(2, HOPS + 1, 2):
        ring_range(a, min(a + 2, HOPS + 1))

    def spreads(early):
        for e in range(SIDE):
            for k in range(2):
                for d in order:
                    a, b = (e, d) if k == 0 else (d, e)
                    c = lax.rem(x + SIDE - a, SIDE) * SIDE + lax.rem(y + SIDE - b, SIDE)
                    m = row_of(c)

                    @pl.when(both((comes_at(m) <= EARLY) == early, second_goes(m, col)))
                    def _():
                        second(k, e, d, m).wait_recv()

    def pairs(s, carry):
        for h in range(CUTS):
            for direction in range(2):
                m = origin(direction, s)

                @pl.when(both(travels(m, direction, s, h), wanted(m)))
                def _():
                    to_pair(direction, s, h, m).wait_recv()

        return carry

    def add(m):
        left = tp[m]
        right = panel[pl.ds(2 * m, 2)].reshape(2 * wr, wc)
        g_ref[...] += lax.dot_general(left, right, (((0,), (0,)), ((), ())), preferred_element_type=F32)

    with jax.named_scope("pairs"):
        spreads(True)
        for k in range(2):
            own_pair(k).wait_recv()
        lax.fori_loop(1, EARLY + 1, pairs, 0)

    def add_blocks(early):
        def step(m, carry):
            @pl.when(both(wanted(m), (comes_at(m) <= EARLY) == early))
            def _():
                add(m)

            return carry

        lax.fori_loop(0, N, step, 0)

    with jax.named_scope("gram"):
        add_blocks(True)

    u_passes(HOPS)
    with jax.named_scope("last"):
        spreads(False)
        lax.fori_loop(EARLY + 1, HOPS + 1, pairs, 0)
        add_blocks(False)
        for direction in range(2):
            for s in range(1, FAR + 1 - direction):
                u_pair(direction, s, origin(direction, s)).wait_recv()
    gb[...] = jnp.transpose(g_ref[...].astype(BF16))

    lanes = wr // 2

    def half_of(k):
        return pl.ds(k * lanes, lanes)

    def line(ref, k, i):
        return ref.at[i, :, :, half_of(k)] if k == 0 else ref.at[:, i, :, half_of(k)]

    def place(k, d):
        return lax.rem((y if k else x) + d, SIDE)

    def reduce1(k, d):
        return copy(
            line(part, k, place(k, d)), row_in.at[k, d - 1], r1_send.at[k, d - 1], r1_recv.at[k, d - 1],
            row, moved(k, d),
        )

    def reduce2(k, d):
        return copy(
            mids.at[k, place(1 - k, d)], last_in.at[k, d - 1], r2_send.at[k, d - 1], r2_recv.at[k, d - 1],
            row, moved(1 - k, d),
        )

    def child_part(i, carry):
        cpl = upanel[pl.ds(2 * SIDE * i, 2 * SIDE)].reshape(SIDE * part.shape[2], wc)
        prod = jnp.dot(cpl, gb[...], preferred_element_type=F32).astype(BF16)
        part[i] = prod.reshape(SIDE, *part.shape[2:])
        return carry

    with jax.named_scope("child"):
        lax.fori_loop(0, SIDE, child_part, 0)
    for d in order:
        for k in range(2):
            reduce1(k, d).start()

    def sent(s, carry):
        for direction in range(2):
            m = origin(direction, s - 1)
            got = origin(direction, s)
            for h in range(CUTS):
                @pl.when(travels(m, direction, s, h))
                def _():
                    hop(direction, s, h, m, False).wait_send()

                @pl.when(both(travels(got, direction, s, h), wanted(got)))
                def _():
                    to_pair(direction, s, h, got).wait_send()

            @pl.when(s < FAR + 1 - direction)
            def _():
                u_hop(direction, s, m, False).wait_send()
                u_pair(direction, s, got).wait_send()

        return carry

    with jax.named_scope("sends"):
        lax.fori_loop(1, HOPS + 1, sent, 0)
        for k in range(2):
            own_pair(k).wait_send()

            @pl.when(both(mirrors(z, col), jnp.logical_not(stays(k, z))))
            def _():
                leg1(k, stage.at[my_rows]).wait_send()

            for e in range(SIDE):
                second_all(k, e, row_of(moved(k, SIDE - e if e else 0)), lambda c: c.wait_send())

        first_all(lambda c: c.wait_send())

        @pl.when(mirrors(z, turn))
        def _():
            leg2().wait_send()

        def handed(h, m, sem_of):
            for k in range(2):
                @pl.when(jnp.logical_not(stays(k, m)))
                def _():
                    hand(k, h, m, w_ref.at[rows_of(h)], sem_of(k)).wait_send()

        @pl.when(col == z)
        def _():
            for h in range(CUTS):
                handed(h, z, lambda k: hand_own.at[h, k])

            def handed_on(s, carry):
                for h in range(CUTS):
                    for direction in range(2):
                        m = origin(direction, s)

                        @pl.when(both(travels(m, direction, s, h), m >= z, s <= NEAR[direction]))
                        def _():
                            handed(h, m, lambda k: hand_send.at[direction, s - 1, h, k])

                return carry

            lax.fori_loop(1, max(NEAR) + 1, handed_on, 0)

    with jax.named_scope("reduce1"):
        for k in range(2):
            mine = part[x, :, :, half_of(k)] if k == 0 else part[:, y, :, half_of(k)]
            sums[k] = mine.astype(F32)
            for d in order:
                reduce1(k, d).wait_recv()
                sums[k] += row_in[k, d - 1].astype(F32)
            mids[k] = sums[k].astype(BF16)
            for d in order:
                reduce2(k, d).start()
    with jax.named_scope("reduce2"):
        for k in range(2):
            total = sums[k, y if k == 0 else x]
            for d in order:
                reduce2(k, d).wait_recv()
                total += last_in[k, d - 1].astype(F32)
            child_ref[:, half_of(k)] = jnp.where(member_ref[:, half_of(k)] > 0, -total, 0.0)
        for k in range(2):
            for d in order:
                reduce1(k, d).wait_send()
                reduce2(k, d).wait_send()


def body(factor, sel_tiles, coupling):
    rows, cols = lax.axis_size("row"), lax.axis_size("col")
    assert rows == 2 * N and cols == N
    wr, wc = factor.shape
    kc = coupling.shape[1]
    row_index = lax.axis_index("row")
    kb = rows * kc // cols
    dma = pltpu.SemaphoreType.DMA
    vm = pl.BlockSpec(memory_space=pltpu.VMEM)
    global_rows = row_index * wr + jnp.arange(wr, dtype=jnp.int32)
    member = jnp.any((global_rows // TILE)[:, None] == sel_tiles[None, :], axis=1)
    pair_of = lambda *shape: [dma(shape), dma(shape)]
    gram, child = pl.pallas_call(
        kernel,
        out_shape=(
            jax.ShapeDtypeStruct((wr, wc), F32),
            jax.ShapeDtypeStruct((kb, wr), F32),
        ),
        in_specs=[vm, vm, vm],
        out_specs=(vm, vm),
        scratch_shapes=[
            pltpu.VMEM((rows, wr, wc), BF16),
            pltpu.VMEM((rows, kc, wc), BF16),
            pltpu.VMEM((cols, 2 * wr, wc // 2), BF16),
            pltpu.VMEM((2 * wr, wc // 2), BF16),
            pltpu.VMEM((wc, wr), BF16),
            pltpu.VMEM((SIDE, SIDE, kb, wr), BF16),
            pltpu.VMEM((2, SIDE, kb, wr // 2), F32),
            pltpu.VMEM((2, SIDE, kb, wr // 2), BF16),
            pltpu.VMEM((2, SIDE - 1, SIDE, kb, wr // 2), BF16),
            pltpu.VMEM((2, SIDE - 1, kb, wr // 2), BF16),
            *pair_of(2, HOPS, CUTS), *pair_of(2, FAR), *pair_of(2, HOPS, CUTS), *pair_of(2, FAR),
            *pair_of(2),
            *pair_of(2), dma, dma, dma((2, max(NEAR), CUTS, 2)), dma((2, CUTS)), dma((CUTS, 2)),
            *pair_of(2, SIDE - 1), *pair_of(2, SIDE, SIDE - 1), *pair_of(2, SIDE - 1), *pair_of(2, SIDE - 1),
        ],
        compiler_params=pltpu.CompilerParams(
            collective_id=0, has_side_effects=True, vmem_limit_bytes=52 * 2**20
        ),
    )(factor, coupling.T, member.astype(F32)[None, :])
    return gram, child


def solution(mesh):
    return jax.shard_map(
        body,
        mesh=mesh,
        in_specs=(P("row", "col"), P(), P("col", "row")),
        out_specs=(P("row", "col"), P("col", "row")),
        check_vma=False,
    )
```

```python
import jax
import jax.numpy as jnp
from jax import lax
from jax.experimental import pallas as pl
from jax.experimental.pallas import tpu as pltpu
from jax.sharding import PartitionSpec as P

TILE = 128
MESH = pl.DeviceIdType.MESH
F32 = jnp.float32
BF16 = jnp.bfloat16
SIDE = 4
N = SIDE * SIDE
FAR = N // 2
SHIFT = 9
CUTS = 2
HOPS = FAR
NEAR = (6, 4)
MIRRORED = 5
EARLY = 4


def both(*conditions):
    out = conditions[0]
    for c in conditions[1:]:
        out = jnp.logical_and(out, c)
    return out


def kernel(
    w_ref, ut_ref, member_ref, g_ref, child_ref,
    panel, upanel, tp, stage, gb, part, sums, mids, row_in, last_in,
    ring_send, ring_recv, u_send, u_recv, pair_send, pair_recv, upair_send, upair_recv,
    own_send, own_recv,
    leg1_send, leg1_recv, leg2_send, leg2_recv, hand_send, hand_recv, hand_own,
    p1_send, p1_recv, p2_send, p2_recv, r1_send, r1_recv, r2_send, r2_recv,
):
    row = lax.axis_index("row")
    col = lax.axis_index("col")
    rows = 2 * N
    core = lax.rem(row, 2)
    z = row // 2
    x = col // SIDE
    y = lax.rem(col, SIDE)
    other = 1 - core
    partner = 2 * z + other
    up = lax.rem(row + 2, rows)
    down = lax.rem(row + rows - 2, rows)
    wr, wc = w_ref.shape
    half = wc // 2
    chunk = wr // CUTS

    def copy(src, dst, ssem, rsem, r, c):
        return pltpu.make_async_remote_copy(
            src_ref=src, dst_ref=dst, send_sem=ssem, recv_sem=rsem,
            device_id=(r, c), device_id_type=MESH,
        )

    def travels(m, direction, s, h):
        near = jnp.logical_or(s < FAR, h % 2 == direction)
        return both(m >= col, m >= FAR if direction == 0 else s <= m, near)

    def gap(m, plane):
        return jnp.where(m - plane <= FAR, m - plane, N - (m - plane))

    def comes_at(m):
        return gap(m, z)

    def wanted(m):
        return both(m >= col, m >= z)

    def origin(direction, s):
        return lax.rem(z + (N - s if direction == 0 else s), N)

    barrier = pltpu.get_barrier_semaphore()

    def greet(r, c):
        pl.semaphore_signal(barrier, inc=1, device_id=(r, c), device_id_type=MESH)

    turn = lax.rem(col + 2 * N - z - SHIFT * core, N)
    for r in (up, down, partner):
        greet(r, col)
    for d in range(1, N):
        greet(row, lax.rem(col + d, N))
    greet(partner, turn)

    @pl.when(turn != z)
    def _():
        greet(2 * turn + core, col)

    @pl.when(col != z)
    def _():
        greet(partner, z)

    with jax.named_scope("barrier"):
        pl.semaphore_wait(barrier, N + 3 + jnp.where(turn != z, 1, 0) + jnp.where(col == z, N - 1, 0))

    def rows_of(h):
        return pl.ds(h * chunk, chunk)

    def towards(direction):
        return up if direction == 0 else down

    def slot_of(m):
        return 2 * m + core

    def hop(direction, s, h, m, first):
        dst = panel.at[slot_of(m), rows_of(h)]
        return copy(
            w_ref.at[rows_of(h)] if first else dst, dst,
            ring_send.at[direction, s - 1, h], ring_recv.at[direction, s - 1, h], towards(direction), col,
        )

    def u_hop(direction, s, m, first):
        dst = upanel.at[slot_of(m)]
        return copy(
            ut_ref if first else dst, dst, u_send.at[direction, s - 1], u_recv.at[direction, s - 1],
            towards(direction), col,
        )

    def to_pair(direction, s, h, m):
        ref = panel.at[slot_of(m), rows_of(h)]
        return copy(
            ref, ref, pair_send.at[direction, s - 1, h], pair_recv.at[direction, s - 1, h], partner, col
        )

    def u_pair(direction, s, m):
        ref = upanel.at[slot_of(m)]
        return copy(ref, ref, upair_send.at[direction, s - 1], upair_recv.at[direction, s - 1], partner, col)

    def own_pair(k):
        src, dst = ((w_ref, panel), (ut_ref, upanel))[k]
        return copy(src, dst.at[row], own_send.at[k], own_recv.at[k], partner, col)

    def part_rows(k):
        return pl.ds(k * wr, wr)

    my_rows = pl.ds(pl.multiple_of(core * wr, wr), wr)

    def leg1(k, dst):
        to = lax.rem(z + col + SHIFT * k, N)
        return copy(
            w_ref.at[:, pl.ds(k * half, half)], dst, leg1_send.at[k], leg1_recv.at[core], 2 * z + k, to
        )

    def stays(k, m):
        return both(core == k, lax.rem(m + SHIFT * k, N) == 0)

    def mirrors(m, plane):
        return both(m - plane > NEAR[1], N - (m - plane) > NEAR[0])

    def leg2():
        return copy(stage, tp.at[z], leg2_send, leg2_recv, 2 * turn + core, col)

    for h in range(CUTS):
        for direction in range(2):
            @pl.when(travels(z, direction, 1, h))
            def _():
                hop(direction, 1, h, z, True).start()

    for k in range(2):
        @pl.when(both(mirrors(z, col), jnp.logical_not(stays(k, z))))
        def _():
            leg1(k, stage.at[my_rows]).start()

        @pl.when(both(mirrors(z, col), stays(k, z)))
        def _():
            stage[my_rows] = w_ref[:, pl.ds(k * half, half)]

    def hand(k, h, m, src, sem):
        return copy(
            src.at[:, pl.ds(k * half, half)],
            tp.at[m, pl.ds(pl.multiple_of(core * wr + h * chunk, chunk), chunk)],
            sem, hand_recv.at[core, h], 2 * z + k, lax.rem(m + z + SHIFT * k, N),
        )

    def hands(h, m, src, sem_of):
        for k in range(2):
            @pl.when(stays(k, m))
            def _():
                tp[m, pl.ds(pl.multiple_of(core * wr + h * chunk, chunk), chunk)] = src[:, pl.ds(k * half, half)]

            @pl.when(jnp.logical_not(stays(k, m)))
            def _():
                hand(k, h, m, src, sem_of(k)).start()

    @pl.when(col == z)
    def _():
        for h in range(CUTS):
            hands(h, z, w_ref.at[rows_of(h)], lambda k: hand_own.at[h, k])

    for direction in range(2):
        u_hop(direction, 1, z, True).start()
    for k in range(2):
        own_pair(k).start()
    panel[row] = w_ref[...]
    upanel[row] = ut_ref[...]
    g_ref[...] = jnp.zeros_like(g_ref)

    def leg1_arrived():
        for k in range(2):
            @pl.when(jnp.logical_not(both(turn == col, core == k)))
            def _():
                copy(
                    w_ref.at[:, pl.ds(0, half)], stage.at[part_rows(k)], leg1_send.at[k], leg1_recv.at[k],
                    row, col,
                ).wait_recv()

    def moved(k, d):
        if k == 0:
            return lax.rem(x + d, SIDE) * SIDE + y
        return x * SIDE + lax.rem(y + d, SIDE)

    def row_of(c):
        return lax.rem(c + 2 * N - z - SHIFT * core, N)

    def least(k, c):
        return c // SIDE * SIDE if k == 0 else lax.rem(c, SIDE)

    def first(k, d, m):
        ref = tp.at[m, part_rows(k)]
        return copy(ref, ref, p1_send.at[k, d - 1], p1_recv.at[k, d - 1], row, moved(k, d))

    def second(k, e, d, m):
        ref = tp.at[m, part_rows(k)]
        return copy(ref, ref, p2_send.at[k, e, d - 1], p2_recv.at[k, e, d - 1], row, moved(1 - k, d))

    def first_goes(k, m, c):
        return both(m >= z, m >= least(k, c))

    def second_goes(m, c):
        return both(m >= z, m >= c)

    order = (1, 3, 2)
    mine = turn

    def first_all(action):
        for d in order:
            for k in range(2):
                @pl.when(first_goes(k, mine, moved(k, d)))
                def _():
                    action(first(k, d, mine))

    def second_all(k, e, m, action):
        for d in order:
            @pl.when(second_goes(m, moved(1 - k, d)))
            def _():
                action(second(k, e, d, m))

    def starts_at(m):
        return jnp.where(mirrors(m, z), MIRRORED, comes_at(m) + 1)

    def spread(s):
        @pl.when(both(mine >= z, starts_at(mine) == s))
        def _():
            @pl.when(mirrors(mine, z))
            def _():
                copy(stage, tp.at[mine], leg2_send, leg2_recv, row, col).wait_recv()

            for k in range(2):
                @pl.when(jnp.logical_not(jnp.logical_or(mirrors(mine, z), both(col == z, core == k))))
                def _():
                    for h in range(CUTS):
                        pltpu.make_async_remote_copy(
                            src_ref=w_ref.at[rows_of(h), pl.ds(0, half)],
                            dst_ref=tp.at[mine, pl.ds(k * wr + h * chunk, chunk)],
                            send_sem=hand_own.at[h, k], recv_sem=hand_recv.at[k, h],
                            device_id=(partner, col), device_id_type=MESH,
                        ).wait_recv()

            first_all(lambda c: c.start())
            for k in range(2):
                second_all(k, 0, mine, lambda c: c.start())

    def relay(s):
        for e in order:
            for k in range(2):
                m = row_of(moved(k, SIDE - e))

                @pl.when(both(starts_at(m) + 1 == s, first_goes(k, m, col)))
                def _():
                    first(k, e, m).wait_recv()
                    second_all(k, e, m, lambda c: c.start())

    def passes(s):
        for h in range(CUTS):
            for direction in range(2):
                m = origin(direction, s)

                @pl.when(travels(m, direction, s, h))
                def _():
                    hop(direction, s, h, m, False).wait_recv()

                    @pl.when(both(s < HOPS, travels(m, direction, s + 1, h)))
                    def _():
                        hop(direction, s + 1, h, m, False).start()

                    @pl.when(wanted(m))
                    def _():
                        to_pair(direction, s, h, m).start()

                    @pl.when(both(col == z, m >= z, s <= NEAR[direction]))
                    def _():
                        src = panel.at[slot_of(m), rows_of(h)]
                        hands(h, m, src, lambda k: hand_send.at[direction, s - 1, h, k])

    def u_passes(s):
        for direction in range(2):
            m = origin(direction, s)

            @pl.when(both(s >= 1, s < FAR + 1 - direction))
            def _():
                u_hop(direction, s, m, False).wait_recv()

                @pl.when(s < FAR - direction)
                def _():
                    u_hop(direction, s + 1, m, False).start()

                u_pair(direction, s, m).start()

    def ring_step(s, carry):
        passes(s)
        u_passes(s - 1)
        spread(s)
        relay(s)
        return carry

    def ring_range(a, b):
        with jax.named_scope("ring%d" % a):
            lax.fori_loop(a, b, ring_step, 0)

    ring_range(1, 2)

    @pl.when(mirrors(z, turn))
    def _():
        with jax.named_scope("leg1"):
            leg1_arrived()
        leg2().start()

    for a in range(2, HOPS + 1, 2):
        ring_range(a, min(a + 2, HOPS + 1))

    def spreads(early):
        for e in range(SIDE):
            for k in range(2):
                for d in order:
                    a, b = (e, d) if k == 0 else (d, e)
                    c = lax.rem(x + SIDE - a, SIDE) * SIDE + lax.rem(y + SIDE - b, SIDE)
                    m = row_of(c)

                    @pl.when(both((comes_at(m) <= EARLY) == early, second_goes(m, col)))
                    def _():
                        second(k, e, d, m).wait_recv()

    def pairs(s, carry):
        for h in range(CUTS):
            for direction in range(2):
                m = origin(direction, s)

                @pl.when(both(travels(m, direction, s, h), wanted(m)))
                def _():
                    to_pair(direction, s, h, m).wait_recv()

        return carry

    def add(m):
        left = tp[m]
        right = panel[pl.ds(2 * m, 2)].reshape(2 * wr, wc)
        g_ref[...] += lax.dot_general(left, right, (((0,), (0,)), ((), ())), preferred_element_type=F32)

    with jax.named_scope("pairs"):
        spreads(True)
        for k in range(2):
            own_pair(k).wait_recv()
        lax.fori_loop(1, EARLY + 1, pairs, 0)

    def add_blocks(early):
        def step(m, carry):
            @pl.when(both(wanted(m), (comes_at(m) <= EARLY) == early))
            def _():
                add(m)

            return carry

        lax.fori_loop(0, N, step, 0)

    with jax.named_scope("gram"):
        add_blocks(True)

    u_passes(HOPS)
    with jax.named_scope("last"):
        spreads(False)
        lax.fori_loop(EARLY + 1, HOPS + 1, pairs, 0)
        add_blocks(False)
        for direction in range(2):
            for s in range(1, FAR + 1 - direction):
                u_pair(direction, s, origin(direction, s)).wait_recv()
    gb[...] = jnp.transpose(g_ref[...].astype(BF16))

    lanes = wr // 2

    def half_of(k):
        return pl.ds(k * lanes, lanes)

    def line(ref, k, i):
        return ref.at[i, :, :, half_of(k)] if k == 0 else ref.at[:, i, :, half_of(k)]

    def place(k, d):
        return lax.rem((y if k else x) + d, SIDE)

    def reduce1(k, d):
        return copy(
            line(part, k, place(k, d)), row_in.at[k, d - 1], r1_send.at[k, d - 1], r1_recv.at[k, d - 1],
            row, moved(k, d),
        )

    def reduce2(k, d):
        return copy(
            mids.at[k, place(1 - k, d)], last_in.at[k, d - 1], r2_send.at[k, d - 1], r2_recv.at[k, d - 1],
            row, moved(1 - k, d),
        )

    def child_part(i, carry):
        cpl = upanel[pl.ds(2 * SIDE * i, 2 * SIDE)].reshape(SIDE * part.shape[2], wc)
        prod = jnp.dot(cpl, gb[...], preferred_element_type=F32).astype(BF16)
        part[i] = prod.reshape(SIDE, *part.shape[2:])
        return carry

    with jax.named_scope("child"):
        lax.fori_loop(0, SIDE, child_part, 0)
    for d in order:
        for k in range(2):
            reduce1(k, d).start()

    def sent(s, carry):
        for direction in range(2):
            m = origin(direction, s - 1)
            got = origin(direction, s)
            for h in range(CUTS):
                @pl.when(travels(m, direction, s, h))
                def _():
                    hop(direction, s, h, m, False).wait_send()

                @pl.when(both(travels(got, direction, s, h), wanted(got)))
                def _():
                    to_pair(direction, s, h, got).wait_send()

            @pl.when(s < FAR + 1 - direction)
            def _():
                u_hop(direction, s, m, False).wait_send()
                u_pair(direction, s, got).wait_send()

        return carry

    with jax.named_scope("sends"):
        lax.fori_loop(1, HOPS + 1, sent, 0)
        for k in range(2):
            own_pair(k).wait_send()

            @pl.when(both(mirrors(z, col), jnp.logical_not(stays(k, z))))
            def _():
                leg1(k, stage.at[my_rows]).wait_send()

            for e in range(SIDE):
                second_all(k, e, row_of(moved(k, SIDE - e if e else 0)), lambda c: c.wait_send())

        first_all(lambda c: c.wait_send())

        @pl.when(mirrors(z, turn))
        def _():
            leg2().wait_send()

        def handed(h, m, sem_of):
            for k in range(2):
                @pl.when(jnp.logical_not(stays(k, m)))
                def _():
                    hand(k, h, m, w_ref.at[rows_of(h)], sem_of(k)).wait_send()

        @pl.when(col == z)
        def _():
            for h in range(CUTS):
                handed(h, z, lambda k: hand_own.at[h, k])

            def handed_on(s, carry):
                for h in range(CUTS):
                    for direction in range(2):
                        m = origin(direction, s)

                        @pl.when(both(travels(m, direction, s, h), m >= z, s <= NEAR[direction]))
                        def _():
                            handed(h, m, lambda k: hand_send.at[direction, s - 1, h, k])

                return carry

            lax.fori_loop(1, max(NEAR) + 1, handed_on, 0)

    with jax.named_scope("reduce1"):
        for k in range(2):
            mine = part[x, :, :, half_of(k)] if k == 0 else part[:, y, :, half_of(k)]
            sums[k] = mine.astype(F32)
            for d in order:
                reduce1(k, d).wait_recv()
                sums[k] += row_in[k, d - 1].astype(F32)
            mids[k] = sums[k].astype(BF16)
            for d in order:
                reduce2(k, d).start()
    with jax.named_scope("reduce2"):
        for k in range(2):
            total = sums[k, y if k == 0 else x]
            for d in order:
                reduce2(k, d).wait_recv()
                total += last_in[k, d - 1].astype(F32)
            child_ref[:, half_of(k)] = jnp.where(member_ref[:, half_of(k)] > 0, -total, 0.0)
        for k in range(2):
            for d in order:
                reduce1(k, d).wait_send()
                reduce2(k, d).wait_send()


def body(factor, sel_tiles, coupling):
    rows, cols = lax.axis_size("row"), lax.axis_size("col")
    assert rows == 2 * N and cols == N
    wr, wc = factor.shape
    kc = coupling.shape[1]
    row_index = lax.axis_index("row")
    kb = rows * kc // cols
    dma = pltpu.SemaphoreType.DMA
    vm = pl.BlockSpec(memory_space=pltpu.VMEM)
    global_rows = row_index * wr + jnp.arange(wr, dtype=jnp.int32)
    member = jnp.any((global_rows // TILE)[:, None] == sel_tiles[None, :], axis=1)
    pair_of = lambda *shape: [dma(shape), dma(shape)]
    gram, child = pl.pallas_call(
        kernel,
        out_shape=(
            jax.ShapeDtypeStruct((wr, wc), F32),
            jax.ShapeDtypeStruct((kb, wr), F32),
        ),
        in_specs=[vm, vm, vm],
        out_specs=(vm, vm),
        scratch_shapes=[
            pltpu.VMEM((rows, wr, wc), BF16),
            pltpu.VMEM((rows, kc, wc), BF16),
            pltpu.VMEM((cols, 2 * wr, wc // 2), BF16),
            pltpu.VMEM((2 * wr, wc // 2), BF16),
            pltpu.VMEM((wc, wr), BF16),
            pltpu.VMEM((SIDE, SIDE, kb, wr), BF16),
            pltpu.VMEM((2, SIDE, kb, wr // 2), F32),
            pltpu.VMEM((2, SIDE, kb, wr // 2), BF16),
            pltpu.VMEM((2, SIDE - 1, SIDE, kb, wr // 2), BF16),
            pltpu.VMEM((2, SIDE - 1, kb, wr // 2), BF16),
            *pair_of(2, HOPS, CUTS), *pair_of(2, FAR), *pair_of(2, HOPS, CUTS), *pair_of(2, FAR),
            *pair_of(2),
            *pair_of(2), dma, dma, dma((2, max(NEAR), CUTS, 2)), dma((2, CUTS)), dma((CUTS, 2)),
            *pair_of(2, SIDE - 1), *pair_of(2, SIDE, SIDE - 1), *pair_of(2, SIDE - 1), *pair_of(2, SIDE - 1),
        ],
        compiler_params=pltpu.CompilerParams(
            collective_id=0, has_side_effects=True, vmem_limit_bytes=52 * 2**20
        ),
    )(factor, coupling.T, member.astype(F32)[None, :])
    return gram, child


def solution(mesh):
    return jax.shard_map(
        body,
        mesh=mesh,
        in_specs=(P("row", "col"), P(), P("col", "row")),
        out_specs=(P("row", "col"), P("col", "row")),
        check_vma=False,
    )
```
